256 devices in a mesh: groups: 2 (over z), expert: 64 (over y, x), tensor: 2 (over core).
Axes of the slice: x: 8, y: 8, z: 2, core: 2. Of those that a mesh axis runs over, the one named last changes fastest.
The devices are a block of a 8x8x16 slice.
Arguments:
- hidden_in: bfloat16 [2048, 3584], P(('groups', 'expert')), parts along dimension 0, may hold values from -6 to 6
- batch_len: int32 [2], P('groups'), parts along dimension 0, may hold values from 256 to 1024
- expert_ids: int32 [2048, 8], P(('groups', 'expert')), parts along dimension 0, may hold values from 0 to 63, all different within a row; in each aligned block of 16 rows (0 to 15, 16 to 31, ...) at most 3 rows name the same one
- gate_num: int32 [2048, 8], P(('groups', 'expert')), parts along dimension 0, may hold values from 1 to 1024
- w_gate: bfloat16 [64, 3584, 1024], P('expert', None, 'tensor'), may hold values from -0.09375 to 0.09375
- w_up: bfloat16 [64, 3584, 1024], P('expert', None, 'tensor'), may hold values from -0.09375 to 0.09375
- w_down: bfloat16 [64, 1024, 3584], P('expert', 'tensor'), may hold values from -0.1875 to 0.1875
- q_latent: bfloat16 [4, 64, 512], P('groups', 'tensor'), parts along dimension 0, may hold values from -117 to 117
- q_rope: bfloat16 [4, 64, 64], P('groups', 'tensor'), parts along dimension 0, may hold values from -6 to 6
- kv_latent: bfloat16 [4, 8192, 512], P('groups', 'expert'), parts along dimension 0, may hold values from -4 to 4
- kv_rope: bfloat16 [4, 64, 8192], P('groups', None, 'expert'), parts along dimension 0, may hold values from -4 to 4
- ctx_len: int32 [4], P('groups'), parts along dimension 0, may hold values from 1 to 8192, as said below
Outputs:
- moe_out: bfloat16 [2048, 3584], P(('groups', 'expert')), parts along dimension 0
- attn_out: bfloat16 [4, 64, 512], P('groups', 'tensor'), parts along dimension 0
The draws below stay inside these ranges and needn't reach their ends.
There are 2 independent parts, one for each index of `groups`. The reference program is written for one: setup_inputs(seed, part) draws one part's arguments, and reference() takes and returns one part's arrays. A program takes and returns all parts, laid end to end along the dimension named above; an argument that names none is the same for every part. Nothing has to cross between parts.
Inputs may be any that keep to these rules, and one draw needn't show every extreme that they name: `expert_ids`: each row names 8 different experts; the 16 rows of one index of the expert axis name any one expert at most 3 times. `batch_len`: the live slots are the first ones of the replica. `ctx_len`: the first request's context fills all 8192 positions.
All inputs are finite; a program needn't handle non-finite values.
Results may differ from the reference program's by a relative error of at most 0.0028.
The reference program's roundings to bfloat16 on the way count: a program that leaves them out, or rounds other values in their place, can miss the bound.
Values may be sent and summed in bfloat16 or wider, within the bound.
No kernel may reach another device: no remote copies, remote signals or barrier semaphores. Data moves between devices by JAX's collectives and lax.ppermute only.
A program may use at most 64 MiB of HBM per device.

```python
import math
import jax
import jax.numpy as jnp
import numpy as np
from jax import lax

D = 3584
FF = 1024
TOPK = 8
H = 64
LAT = 512
ROPE = 64
TOK_DEV = 16
BATCH = 2
EXPERTS = 64
TOKENS = 1024
CAP = 3
CTX = 8192
N_EXPERT = 64


def cache_pair(key):
    base = jax.random.fold_in(key, 71)
    first, second = jax.random.split(base)
    latent = jax.random.truncated_normal(first, -4.0, 4.0, (BATCH, CTX, LAT), jnp.float32)
    rotary = jax.random.truncated_normal(second, -4.0, 4.0, (BATCH, ROPE, CTX), jnp.float32)
    return (latent, rotary)


def draw_kv_latent(key, part):
    return cache_pair(key)[0].astype(jnp.bfloat16)


def draw_kv_rope(key, part):
    return cache_pair(key)[1].astype(jnp.bfloat16)


def draw_ctx_len(key, part):
    lengths = jax.random.randint(jax.random.fold_in(key, 53), (BATCH,), 1, CTX + 1, dtype=jnp.int32)
    first = jnp.arange(BATCH, dtype=jnp.int32) == 0
    return jnp.where(first, CTX, lengths).astype(jnp.int32)


def draw_q_latent(key, part):
    noise = jax.random.truncated_normal(jax.random.fold_in(key, 37), -4.0, 4.0, (BATCH, H, LAT), jnp.float32)
    latent = cache_pair(key)[0]
    head_anchor = latent[:, 0, :] + latent[:, 1, :]
    tail_anchor = latent[:, CTX - 2, :] + latent[:, CTX - 1, :]
    first = (jnp.arange(BATCH, dtype=jnp.int32) == 0)[:, None]
    anchor = jnp.where(first, tail_anchor, head_anchor)
    length_sq = jnp.sum(anchor * anchor, axis=1) + 1.0
    heads = jnp.arange(H, dtype=jnp.int32)
    strength = 250.0 + 150.0 * (heads // 2 % 3).astype(jnp.float32)
    chosen = heads % 2 == 0
    direction = anchor * 192.0 ** 0.5 / length_sq[:, None]
    aligned = strength[None, :, None] * direction[:, None, :]
    mixed = jnp.where(chosen[None, :, None], aligned, noise)
    bound = float(60000 // LAT)
    return jnp.clip(mixed, -bound, bound).astype(jnp.bfloat16)


def touch_ends(drawn, own_key, smallest, top_value):
    dims = drawn.shape
    spot = [jax.random.randint(jax.random.fold_in(own_key, axis), (), 0, dims[axis]) for axis in range(len(dims))]
    drawn = drawn.at[tuple(spot)].set(smallest)
    longest = dims.index(max(dims))
    spot[longest] = (spot[longest] + 1) % dims[longest]
    return drawn.at[tuple(spot)].set(top_value)


def block_levels(own_key, extent, pieces, low, largest):
    def one(axis_at, shards_of):
        draws = jax.random.uniform(jax.random.fold_in(jax.random.fold_in(own_key, 6), axis_at), (shards_of,), jnp.float32, low / len(pieces), largest / len(pieces))
        return jnp.repeat(jnp.exp(draws), extent[axis_at] // shards_of).reshape((-1,) + (1,) * (len(extent) - axis_at - 1))

    factor_of = one(*pieces[0])
    for cut in pieces[1:]:
        factor_of = factor_of * one(*cut)
    return factor_of


def assign_block(stream_key, own, number, rows, count, top, reach, slope):
    order = jax.random.permutation(stream_key, count)
    heavy_load, ordinary = shares(count, rows * top, reach, slope, True), shares(count, rows * top, reach, slope, False)
    places = jnp.arange(count)

    def named(sizes, offset_by):
        used = int((sizes > 0).sum())
        fixed = max(1, used // 4)
        shifted = fixed + (places - fixed + offset_by * (used - fixed)) % max(1, count - fixed)
        return jnp.zeros((count,), jnp.int32).at[order[jnp.where(places < fixed, places, shifted)]].set(jnp.asarray(sizes, jnp.int32))

    sizes = jnp.where(number % 4 == 0, named(heavy_load, number // 4), named(ordinary, number - number // 4 - 1))
    mixed = jax.random.permutation(jax.random.fold_in(own, 3), count)
    donor, taker = mixed[0:count // 2 * 2:2], mixed[1:count // 2 * 2:2]
    margin = jnp.minimum(sizes[donor] - 1, reach - sizes[taker]) // 2
    margin = jnp.where((donor == order[0]) | (taker == order[0]) | (sizes[taker] == 0), 0, jnp.maximum(margin, 0))
    shifted = jax.random.randint(jax.random.fold_in(own, 4), (count // 2,), 0, 1 << 20) % (margin + 1)
    sizes = sizes.at[donor].add(-shifted).at[taker].add(shifted)
    items = jnp.searchsorted(jnp.cumsum(sizes), jnp.arange(rows * top), side="right").astype(jnp.int32)
    listing = items.reshape(top, rows).T
    listing = listing[jax.random.permutation(jax.random.fold_in(own, 1), rows)]
    offset_by = jax.random.randint(jax.random.fold_in(own, 2), (rows, 1), 0, top)
    return jnp.take_along_axis(listing, (jnp.arange(top)[None, :] + offset_by) % top, axis=1)


def shares(count, total, most, skew, full):
    loads = [(1 << 20) // math.isqrt(grade ** skew) + 1 for grade in range(1, count + 1)]
    largest = most if full else min(most, max(-(-total // count), total * loads[0] // sum(loads)))
    least = 1 if total - largest >= count - 1 else 0
    holding, rest = [largest] + [least] * (count - 1), total - largest - least * (count - 1)
    while rest > 0:
        free = [i for i in range(1, count) if holding[i] < largest] or [i for i in range(1, count) if holding[i] < most]
        pool, budget = sum([loads[i] for i in free]), rest
        for i in free:
            more = min(most - holding[i], max(1, budget * loads[i] // pool), rest)
            holding[i] = holding[i] + more
            rest = rest - more
    return np.array(holding)


def gaussian(stream_key, shape, width, reach, cuts=(), kind=jnp.bfloat16):
    values = width * jax.random.normal(stream_key, shape, jnp.float32)
    if cuts:
        values = values * block_levels(stream_key, shape, cuts, -0.22, 0.18)
    return jnp.clip(values, -reach, reach).astype(kind)


def setup_inputs(seed: int = 0, part: int = 0) -> dict:
    key_of = jax.random.split(jax.random.key(seed), 13)
    own_keys = jax.random.split(jax.random.fold_in(key_of[12], part), 13)
    hidden_in = gaussian(own_keys[0], (TOKENS, D), 1.0, 6.0, ((0, 64),))
    batch_len = jax.random.randint(own_keys[1], (1,), TOKENS // 4, TOKENS + 1).astype(jnp.int32)
    expert_ids_keys = jax.random.split(jax.random.fold_in(own_keys[2], 1), TOKENS // TOK_DEV)
    expert_ids_turns = jax.random.permutation(jax.random.fold_in(own_keys[2], 3), TOKENS // TOK_DEV)
    expert_ids = jax.vmap(lambda own, number: assign_block(jax.random.fold_in(own_keys[2], 2), own, number, TOK_DEV, EXPERTS, TOPK, CAP, 2))(expert_ids_keys, expert_ids_turns).reshape((TOKENS, TOPK))
    gate_num = touch_ends(jax.random.randint(own_keys[3], (TOKENS, TOPK), 1, 1025), jax.random.fold_in(own_keys[3], 1), 1, 1024).astype(jnp.int32)
    w_gate = gaussian(key_of[4], (EXPERTS, D, FF), D ** -0.5, 0.09375, ((0, 64), (2, 2)))
    w_up = gaussian(key_of[5], (EXPERTS, D, FF), D ** -0.5, 0.09375, ((0, 64), (2, 2)))
    w_down = gaussian(key_of[6], (EXPERTS, FF, D), FF ** -0.5, 0.1875, ((0, 64), (1, 2)))
    q_latent = draw_q_latent(jax.random.fold_in(jax.random.fold_in(key_of[12], part), 71), part)
    q_rope = gaussian(own_keys[8], (BATCH, H, ROPE), 1.0, 6.0, ((1, 2),))
    kv_latent = draw_kv_latent(jax.random.fold_in(jax.random.fold_in(key_of[12], part), 71), part)
    kv_rope = draw_kv_rope(jax.random.fold_in(jax.random.fold_in(key_of[12], part), 71), part)
    ctx_len = draw_ctx_len(jax.random.fold_in(jax.random.fold_in(key_of[12], part), 71), part)
    return dict(hidden_in=hidden_in, batch_len=batch_len, expert_ids=expert_ids, gate_num=gate_num, w_gate=w_gate, w_up=w_up, w_down=w_down, q_latent=q_latent, q_rope=q_rope, kv_latent=kv_latent, kv_rope=kv_rope, ctx_len=ctx_len)


gate_denominator = 1024.0
softmax_scale = 192.0 ** -0.5


def reference(hidden_in, batch_len, expert_ids, gate_num, w_gate, w_up, w_down, q_latent, q_rope, kv_latent, kv_rope, ctx_len):
    live = jnp.arange(TOKENS, dtype=jnp.int32) < batch_len[0]
    flat_expert = expert_ids.reshape(-1)
    token_of = jnp.arange(TOKENS * TOPK, dtype=jnp.int32) // TOPK
    live_pick = live[token_of]
    weight = jnp.where(live_pick, gate_num.reshape(-1).astype(jnp.float32) / gate_denominator, 0.0)
    rows_most = N_EXPERT * CAP

    def one_expert(total, index):
        match = (flat_expert == index) & live_pick
        picked = jnp.nonzero(match, size=rows_most, fill_value=0)[0].astype(jnp.int32)
        valid = jnp.arange(rows_most, dtype=jnp.int32) < jnp.sum(match.astype(jnp.int32))
        tokens = token_of[picked]
        rows = hidden_in[tokens]
        gate = jnp.dot(rows, w_gate[index], preferred_element_type=jnp.float32)
        upper = jnp.dot(rows, w_up[index], preferred_element_type=jnp.float32)
        hidden = (jax.nn.silu(gate) * upper).astype(jnp.bfloat16)
        value = jnp.dot(hidden, w_down[index], preferred_element_type=jnp.float32).astype(jnp.bfloat16)
        value = lax.optimization_barrier(value).astype(jnp.float32)
        scaled = value * jnp.where(valid, weight[picked], 0.0)[:, None]
        return total.at[tokens].add(scaled), None

    start = jnp.zeros((TOKENS, D), jnp.float32)
    summed, unused = lax.scan(one_expert, start, jnp.arange(EXPERTS, dtype=jnp.int32))
    moe_out = summed.astype(jnp.bfloat16)

    scores = jnp.einsum("bhl,bpl->bhp", q_latent.astype(jnp.float32), kv_latent.astype(jnp.float32))
    scores = scores + jnp.einsum("bhr,brp->bhp", q_rope.astype(jnp.float32), kv_rope.astype(jnp.float32))
    scores = scores * softmax_scale
    valid_pos = jnp.arange(CTX, dtype=jnp.int32)[None, :] < ctx_len[:, None]
    scores = jnp.where(valid_pos[:, None, :], scores, -1e30)
    top = jnp.max(scores, axis=2, keepdims=True)
    probs = jnp.where(valid_pos[:, None, :], jnp.exp(scores - top), 0.0)
    total = jnp.sum(probs, axis=2, keepdims=True)
    probs_bf = lax.optimization_barrier(probs.astype(jnp.bfloat16)).astype(jnp.float32)
    weighted = jnp.einsum("bhp,bpl->bhl", probs_bf, kv_latent.astype(jnp.float32))
    attn_out = (weighted / total).astype(jnp.bfloat16)
    return moe_out, attn_out
```

```python
import functools

import jax
import jax.numpy as jnp
from jax import lax
from jax.experimental import pallas as pl
from jax.experimental.pallas import tpu as pltpu
from jax.sharding import PartitionSpec as P

SUB = 8
CAP = 3
bf16 = jnp.bfloat16
f32 = jnp.float32
softmax_scale = 192.0 ** (-0.5)
gate_denominator = 1024.0
INTERPRET = False


def iota(shape, dim):
    return lax.broadcasted_iota(jnp.int32, shape, dim)


def dot(a, b):
    return jnp.dot(a, b, preferred_element_type=f32)


def dot_nt(a, b):
    return lax.dot_general(a, b, (((1,), (1,)), ((), ())), preferred_element_type=f32)


def ones_where(condition, dtype=bf16):
    return jnp.where(condition, 1.0, 0.0).astype(dtype)


def in_three(value):
    high = value.astype(bf16).astype(f32)
    middle = (value - high).astype(bf16).astype(f32)
    return high, middle, (value - high - middle).astype(bf16).astype(f32)


def routing(ids, owners, first_row, live_count):
    rows, topk = ids.shape
    lane = iota((rows, owners), 1)
    picks = [ids[:, k : k + 1] == lane for k in range(topk)]
    live = first_row + iota((rows, owners), 0) < live_count
    match = sum(ones_where(p, f32) for p in picks)
    match = jnp.where(live, match, 0.0)
    before = ones_where(iota((rows, rows), 1) < iota((rows, rows), 0))
    return picks, match, dot(before, match.astype(bf16))


def pack_kernel(where_ref, len_ref, ctx_ref, hid_ref, ids_ref, ql_ref, qr_ref, kl_ref, kr_ref, out_ref):
    expert, tensor = where_ref[0], where_ref[1]
    total_rows, width = out_ref.shape
    owners = total_rows // SUB
    piece = width // CAP
    tok = hid_ref.shape[0]
    half = hid_ref.shape[1] // 2
    batch, heads, lat = ql_ref.shape
    ctx_dev = kl_ref.shape[1]

    parts = []
    for b in range(batch):
        latent = kl_ref[b]
        s = dot_nt(ql_ref[b], latent) + dot(qr_ref[b], kr_ref[b])
        valid = expert * ctx_dev + iota((heads, ctx_dev), 1) < ctx_ref[b]
        s = jnp.where(valid, s * softmax_scale, -1e30)
        top = jnp.max(s, axis=1, keepdims=True)
        p = jnp.where(valid, jnp.exp(s - top), 0.0)
        total = jnp.sum(p, axis=1, keepdims=True)
        mean = dot(p.astype(bf16), latent) / jnp.where(total > 0.0, total, 1.0)
        at = iota((heads, width - lat), 1)
        stats = jnp.zeros((heads, width - lat), f32)
        for k, number in enumerate(in_three(top) + in_three(total)):
            stats = jnp.where(at == k, number, stats)
        parts.append(jnp.concatenate([mean, stats], axis=1).astype(bf16))
    attn = jnp.concatenate(parts, axis=0)

    hidden = hid_ref[...]
    source = jnp.where(tensor == 0, hidden[:, :half], hidden[:, half:])
    stacked = [source[:, k * piece : (k + 1) * piece] for k in range(half // piece)]
    stacked.append(jnp.zeros((tok, piece), bf16))
    stacked = jnp.concatenate(stacked, axis=0)
    _, match, rank = routing(ids_ref[...], owners, expert * tok, len_ref[0])
    mine = [jnp.where(rank == c, match, 0.0).astype(bf16) for c in range(CAP)]
    tiled = jnp.concatenate([m for m in mine for _ in range(SUB)], axis=0)
    spread = ones_where(iota((total_rows, owners), 0) // SUB == iota((total_rows, owners), 1))
    chosen = dot_nt(spread, tiled)
    block = SUB * tok
    row, col = iota((total_rows, block), 0), iota((total_rows, block), 1)
    kept = (row % SUB == col // tok) & (col < block - tok)
    last = ones_where(
        iota((total_rows, owners), 0) == iota((total_rows, owners), 1) * SUB + (SUB - 1)
    )
    for c in range(CAP):
        lhs = jnp.where(kept, chosen[:, c * block : (c + 1) * block], 0.0).astype(bf16)
        at = slice(c * piece, (c + 1) * piece)
        out_ref[:, at] = (dot(lhs, stacked) + dot(last, attn[:, at])).astype(bf16)


def ffn_kernel(
    where_ref, own_ref, other_ref, wg_ref, wu_ref, wd_ref,
    keep_ref, send_ref, attn_ref,
    wg, wu, wd, rows, sems,
):
    tensor = where_ref[1]
    total_rows, width = own_ref.shape
    owners = total_rows // SUB
    piece = width // CAP
    half = wg_ref.shape[1] // 2
    lat = attn_ref.shape[1]
    first = [pl.multiple_of(tensor * half, half), pl.multiple_of((1 - tensor) * half, half)]

    copies = []
    for h in range(2):
        copies.append(pltpu.make_async_copy(wg_ref.at[0, pl.ds(first[h], half), :], wg.at[h], sems.at[2 * h]))
        copies.append(pltpu.make_async_copy(wu_ref.at[0, pl.ds(first[h], half), :], wu.at[h], sems.at[2 * h + 1]))
    for h in range(2):
        copies.append(pltpu.make_async_copy(wd_ref.at[0, :, pl.ds(first[1 - h], half)], wd.at[1 - h], sems.at[4 + h]))
    for copy in copies:
        copy.start()

    row, col = iota((total_rows, total_rows), 0), iota((total_rows, total_rows), 1)
    order = ones_where(col == (row % owners) * SUB + row // owners)
    for h, ref in enumerate((own_ref, other_ref)):
        sorted_rows = dot(order, ref[...])
        for k in range(SUB - 1):
            for c in range(CAP):
                rows[h, c * owners : (c + 1) * owners, k * piece : (k + 1) * piece] = sorted_rows[
                    k * owners : (k + 1) * owners, c * piece : (c + 1) * piece
                ].astype(bf16)
        if h == 0:
            arrived = sorted_rows[(SUB - 1) * owners :]
            stats = [arrived[:, lat + k : lat + k + 1] for k in range(6)]
            top = stats[0] + stats[1] + stats[2]
            total = stats[3] + stats[4] + stats[5]
            share = jnp.exp(top - jnp.max(top, axis=0, keepdims=True)) * total
            weighted = jnp.sum(share * arrived[:, :lat], axis=0, keepdims=True)
            done = weighted / jnp.sum(share, axis=0, keepdims=True)
            attn_ref[...] = jnp.broadcast_to(done, attn_ref.shape).astype(bf16)

    copies[0].wait()
    gate = dot(rows[0], wg[0])
    copies[1].wait()
    upper = dot(rows[0], wu[0])
    copies[2].wait()
    gate = gate + dot(rows[1], wg[1])
    copies[3].wait()
    upper = upper + dot(rows[1], wu[1])
    hidden = (gate / (1.0 + jnp.exp(-gate)) * upper).astype(bf16)
    copies[4].wait()
    send_ref[...] = dot(hidden, wd[1])
    copies[5].wait()
    keep_ref[...] = dot(hidden, wd[0])


def back_kernel(keep_ref, come_ref, attn_ref, out_ref, value):
    total_rows, width = out_ref.shape
    owners = total_rows // SUB
    piece = width // CAP
    lat = attn_ref.shape[1]
    for k in range(SUB - 1):
        for c in range(CAP):
            at = (slice(c * owners, (c + 1) * owners), slice(k * piece, (k + 1) * piece))
            value[k * owners : (k + 1) * owners, c * piece : (c + 1) * piece] = (
                keep_ref[at] + come_ref[at]
            ).astype(bf16)
    value[(SUB - 1) * owners :, :lat] = jnp.broadcast_to(attn_ref[0:1, :], (owners, lat))
    value[(SUB - 1) * owners :, lat:] = jnp.zeros((owners, width - lat), bf16)
    row, col = iota((total_rows, total_rows), 0), iota((total_rows, total_rows), 1)
    order = ones_where(col == (row % SUB) * owners + row // SUB)
    out_ref[...] = dot(order, value[...]).astype(bf16)


def sum_kernel(where_ref, len_ref, back_ref, ids_ref, gate_ref, moe_ref, attn_ref):
    expert = where_ref[0]
    total_rows, width = back_ref.shape
    owners = total_rows // SUB
    piece = width // CAP
    tok = ids_ref.shape[0]
    picks, match, rank = routing(ids_ref[...], owners, expert * tok, len_ref[0])
    gates = gate_ref[...]
    lower = gates % 8
    split = []
    for number in (gates - lower, lower):
        number = number.astype(f32)
        split.append(sum(jnp.where(p, number[:, k : k + 1], 0.0) for k, p in enumerate(picks)))
    spread = ones_where(iota((total_rows, owners), 0) // SUB == iota((total_rows, owners), 1))
    tiled = []
    for c in range(CAP):
        for number in split:
            mine = jnp.where((rank == c) & (match > 0.0), number, 0.0).astype(bf16)
            tiled.extend([mine] * SUB)
    chosen = dot_nt(jnp.concatenate(tiled, axis=0), spread)
    block = SUB * tok
    row, col = iota((2 * block, total_rows), 0), iota((2 * block, total_rows), 1)
    kept = row % block // tok == col % SUB
    summed = jnp.zeros((2 * block, piece), f32)
    for c in range(CAP):
        lhs = jnp.where(kept, chosen[c * 2 * block : (c + 1) * 2 * block], 0.0).astype(bf16)
        summed = summed + dot(lhs, back_ref[:, c * piece : (c + 1) * piece])
    summed = (summed[:block] + summed[block:]) * (1.0 / gate_denominator)
    for k in range(SUB - 1):
        moe_ref[:, k * piece : (k + 1) * piece] = summed[k * tok : (k + 1) * tok].astype(bf16)
    lat = attn_ref.shape[1]
    last = ones_where(
        iota((owners, total_rows), 1) == iota((owners, total_rows), 0) * SUB + (SUB - 1)
    )
    attn_ref[...] = dot(last, back_ref[:, :lat]).astype(bf16)


def vmem():
    return pl.BlockSpec(memory_space=pltpu.VMEM)


def smem():
    return pl.BlockSpec(memory_space=pltpu.SMEM)


def hbm():
    return pl.BlockSpec(memory_space=pl.ANY)


def call(kernel, out_shape, in_specs, scratch=(), vmem_mib=32):
    several = isinstance(out_shape, (tuple, list))
    return pl.pallas_call(
        kernel,
        out_shape=out_shape,
        in_specs=in_specs,
        out_specs=tuple(vmem() for _ in out_shape) if several else vmem(),
        scratch_shapes=list(scratch),
        compiler_params=pltpu.CompilerParams(vmem_limit_bytes=vmem_mib << 20),
        interpret=INTERPRET,
    )


def local(
    hidden_in,
    batch_len,
    expert_ids,
    gate_num,
    w_gate,
    w_up,
    w_down,
    q_latent,
    q_rope,
    kv_latent,
    kv_rope,
    ctx_len,
):
    owners = lax.axis_size("expert")
    tok, features = hidden_in.shape
    half = features // 2
    hidden_units = w_gate.shape[2]
    batch, heads, lat = q_latent.shape
    total_rows = owners * SUB
    width = CAP * half // (SUB - 1)
    tensor = lax.axis_index("tensor")
    where = jnp.stack([lax.axis_index("expert"), tensor]).astype(jnp.int32)
    swap = [(0, 1), (1, 0)]

    def exchanged(packed):
        whole = packed.reshape(owners, SUB, width)
        return lax.all_to_all(whole, "expert", 0, 0, tiled=True).reshape(total_rows, width)

    packed = call(
        pack_kernel,
        jax.ShapeDtypeStruct((total_rows, width), bf16),
        [smem(), smem(), smem(), vmem(), vmem(), vmem(), vmem(), vmem(), vmem()],
    )(where, batch_len, ctx_len, hidden_in, expert_ids, q_latent, q_rope, kv_latent, kv_rope)
    own = exchanged(packed)
    other = lax.ppermute(own, "tensor", swap)
    slots = CAP * owners
    keep, send, attn = call(
        ffn_kernel,
        (
            jax.ShapeDtypeStruct((slots, half), f32),
            jax.ShapeDtypeStruct((slots, half), f32),
            jax.ShapeDtypeStruct((16, lat), bf16),
        ),
        [smem(), vmem(), vmem(), hbm(), hbm(), hbm()],
        [
            pltpu.VMEM((2, half, hidden_units), bf16),
            pltpu.VMEM((2, half, hidden_units), bf16),
            pltpu.VMEM((2, hidden_units, half), bf16),
            pltpu.VMEM((2, slots, half), bf16),
            pltpu.SemaphoreType.DMA((6,)),
        ],
        48,
    )(where, own, other, w_gate, w_up, w_down)
    come = lax.ppermute(send, "tensor", swap)
    returned = call(
        back_kernel,
        jax.ShapeDtypeStruct((total_rows, width), bf16),
        [vmem(), vmem(), vmem()],
        [pltpu.VMEM((total_rows, width), bf16)],
    )(keep, come, attn)
    back = exchanged(returned)
    moe_half, attn_out = call(
        sum_kernel,
        (
            jax.ShapeDtypeStruct((tok, half), bf16),
            jax.ShapeDtypeStruct((batch * heads, lat), bf16),
        ),
        [smem(), smem(), vmem(), vmem(), vmem()],
    )(where, batch_len, back, expert_ids, gate_num)
    moe_other = lax.ppermute(moe_half, "tensor", swap)
    moe_out = jnp.where(
        tensor == 0,
        jnp.concatenate([moe_half, moe_other], axis=1),
        jnp.concatenate([moe_other, moe_half], axis=1),
    )
    return moe_out, attn_out.reshape(batch, heads, lat)


def solution(mesh):
    both = ("groups", "expert")
    in_specs = (
        P(both, None),
        P("groups"),
        P(both, None),
        P(both, None),
        P("expert", None, "tensor"),
        P("expert", None, "tensor"),
        P("expert", "tensor", None),
        P("groups", "tensor", None),
        P("groups", "tensor", None),
        P("groups", "expert", None),
        P("groups", None, "expert"),
        P("groups"),
    )
    out_specs = (P(both, None), P("groups", "tensor", None))
    return jax.shard_map(local, mesh=mesh, in_specs=in_specs, out_specs=out_specs, check_vma=False)
```

```python
import functools

import jax
import jax.numpy as jnp
from jax import lax
from jax.experimental import pallas as pl
from jax.experimental.pallas import tpu as pltpu
from jax.sharding import PartitionSpec as P

SUB = 8
CAP = 3
bf16 = jnp.bfloat16
f32 = jnp.float32
softmax_scale = 192.0 ** (-0.5)
gate_denominator = 1024.0
INTERPRET = False


def iota(shape, dim):
    return lax.broadcasted_iota(jnp.int32, shape, dim)


def dot(a, b):
    return jnp.dot(a, b, preferred_element_type=f32)


def dot_nt(a, b):
    return lax.dot_general(a, b, (((1,), (1,)), ((), ())), preferred_element_type=f32)


def ones_where(condition, dtype=bf16):
    return jnp.where(condition, 1.0, 0.0).astype(dtype)


def in_three(value):
    high = value.astype(bf16).astype(f32)
    middle = (value - high).astype(bf16).astype(f32)
    return high, middle, (value - high - middle).astype(bf16).astype(f32)


def routing(ids_t, owners, tok, live_count):
    topk = ids_t.shape[0]
    lanes = SUB * tok
    repeat = ones_where(iota((tok, lanes), 1) % tok == iota((tok, lanes), 0))
    ids = dot(ids_t.astype(f32).astype(bf16), repeat)
    row = iota((owners, lanes), 0).astype(f32)
    picks = [ids[k : k + 1, :] == row for k in range(topk)]
    live = lax.axis_index("expert") * tok + iota((owners, lanes), 1) % tok < live_count
    match = sum(ones_where(p, f32) for p in picks)
    match = jnp.where(live, match, 0.0)
    first, second = iota((lanes, lanes), 0), iota((lanes, lanes), 1)
    before = ones_where((first // tok == second // tok) & (first < second))
    return repeat, picks, match, dot(match.astype(bf16), before)


def pack_kernel(
    len_ref, ctx_ref, hid_hbm, ids_hbm, ql_hbm, qr_hbm, kl_hbm, kr_hbm,
    out_ref,
    hid_ref, ids_ref, ql_ref, qr_ref, kl_ref, kr_ref, sems,
):
    pairs = (
        (ql_hbm, ql_ref), (kl_hbm, kl_ref), (qr_hbm, qr_ref),
        (kr_hbm, kr_ref), (ids_hbm, ids_ref), (hid_hbm, hid_ref),
    )
    copies = copied(pairs, sems)
    expert, tensor = lax.axis_index("expert"), lax.axis_index("tensor")
    total_rows, width = out_ref.shape
    owners = total_rows // SUB
    piece = width // CAP
    tok = hid_ref.shape[0]
    half = hid_ref.shape[1] // 2
    batch, heads, lat = ql_ref.shape
    ctx_dev = kl_ref.shape[1]

    block = SUB * tok
    row, col = iota((total_rows, block), 0), iota((total_rows, block), 1)
    kept = (row % SUB == col // tok) & (col < block - tok)
    spread = ones_where(iota((total_rows, owners), 0) // SUB == iota((total_rows, owners), 1))
    last = ones_where(
        iota((total_rows, owners), 0) == iota((total_rows, owners), 1) * SUB + (SUB - 1)
    )
    for copy in copies[:4]:
        copy.wait()
    parts = []
    for b in range(batch):
        latent = kl_ref[b]
        s = dot_nt(ql_ref[b], latent) + dot(qr_ref[b], kr_ref[b])
        valid = expert * ctx_dev + iota((heads, ctx_dev), 1) < ctx_ref[b]
        s = jnp.where(valid, s * softmax_scale, -1e30)
        top = jnp.max(s, axis=1, keepdims=True)
        p = jnp.where(valid, jnp.exp(s - top), 0.0)
        total = jnp.sum(p, axis=1, keepdims=True)
        mean = dot(p.astype(bf16), latent) / jnp.where(total > 0.0, total, 1.0)
        at = iota((heads, width - lat), 1)
        stats = jnp.zeros((heads, width - lat), f32)
        for k, number in enumerate(in_three(top) + in_three(total)):
            stats = jnp.where(at == k, number, stats)
        parts.append(jnp.concatenate([mean, stats], axis=1).astype(bf16))
    attn = jnp.concatenate(parts, axis=0)

    for copy in copies[4:]:
        copy.wait()
    _, _, match, rank = routing(ids_ref[...], owners, tok, len_ref[0])
    hidden = hid_ref[...]
    source = jnp.where(tensor == 0, hidden[:, :half], hidden[:, half:])
    stacked = [source[:, k * piece : (k + 1) * piece] for k in range(half // piece)]
    stacked.append(jnp.zeros((tok, piece), bf16))
    stacked = jnp.concatenate(stacked, axis=0)
    for c in range(CAP):
        mine = jnp.where(rank == c, match, 0.0).astype(bf16)
        lhs = jnp.where(kept, dot(spread, mine), 0.0).astype(bf16)
        at = slice(c * piece, (c + 1) * piece)
        out_ref[:, at] = (dot(lhs, stacked) + dot(last, attn[:, at])).astype(bf16)


def sort_rows(arrived, rows):
    total_rows, width = arrived.shape
    owners = total_rows // SUB
    piece = width // CAP
    row, col = iota((total_rows, total_rows), 0), iota((total_rows, total_rows), 1)
    order = ones_where(col == (row % owners) * SUB + row // owners)
    ordered = dot(order, arrived)
    for k in range(SUB - 1):
        for c in range(CAP):
            rows[c * owners : (c + 1) * owners, k * piece : (k + 1) * piece] = ordered[
                k * owners : (k + 1) * owners, c * piece : (c + 1) * piece
            ].astype(bf16)
    return ordered[(SUB - 1) * owners :]


def copied(pairs, sems):
    copies = [pltpu.make_async_copy(a, b, sems.at[k]) for k, (a, b) in enumerate(pairs)]
    for copy in copies:
        copy.start()
    return copies


def own_kernel(
    own_ref, wg_hbm, wu_hbm,
    gate_ref, upper_ref, attn_ref, next_gate_ref, next_up_ref,
    wg, wu, rows, sems,
):
    half = rows.shape[1]
    lat = attn_ref.shape[1]
    tensor = lax.axis_index("tensor")
    mine = pl.ds(pl.multiple_of(tensor * half, half), half)
    theirs = pl.ds(pl.multiple_of((1 - tensor) * half, half), half)
    copies = copied(
        (
            (wg_hbm.at[0, mine, :], wg),
            (wu_hbm.at[0, mine, :], wu),
            (wg_hbm.at[0, theirs, :], next_gate_ref),
            (wu_hbm.at[0, theirs, :], next_up_ref),
        ),
        sems,
    )
    arrived = sort_rows(own_ref[...], rows)
    stats = [arrived[:, lat + k : lat + k + 1] for k in range(6)]
    top = stats[0] + stats[1] + stats[2]
    total = stats[3] + stats[4] + stats[5]
    share = jnp.exp(top - jnp.max(top, axis=0, keepdims=True)) * total
    weighted = jnp.sum(share * arrived[:, :lat], axis=0, keepdims=True)
    done = weighted / jnp.sum(share, axis=0, keepdims=True)
    attn_ref[...] = jnp.broadcast_to(done, attn_ref.shape).astype(bf16)
    copies[0].wait()
    gate_ref[...] = dot(rows[...], wg[...])
    copies[1].wait()
    upper_ref[...] = dot(rows[...], wu[...])
    copies[2].wait()
    copies[3].wait()


def other_kernel(
    other_ref, wg_ref, wu_ref, gate_ref, upper_ref, wd_hbm,
    hidden_ref, next_down_ref,
    rows, sems,
):
    half = rows.shape[1]
    mine = pl.ds(pl.multiple_of(lax.axis_index("tensor") * half, half), half)
    copies = copied(((wd_hbm.at[0, :, mine], next_down_ref),), sems)
    sort_rows(other_ref[...], rows)
    gate = gate_ref[...] + dot(rows[...], wg_ref[...])
    upper = upper_ref[...] + dot(rows[...], wu_ref[...])
    hidden_ref[...] = (gate / (1.0 + jnp.exp(-gate)) * upper).astype(bf16)
    copies[0].wait()


def down_kernel(hidden_ref, wd_ref, sum_ref):
    sum_ref[...] = dot(hidden_ref[...], wd_ref[...])


def back_kernel(sum_ref, hidden_ref, wd_ref, attn_ref, out_ref, rows):
    total_rows, width = out_ref.shape
    owners = total_rows // SUB
    piece = width // CAP
    lat = attn_ref.shape[1]
    whole = (sum_ref[...] + dot(hidden_ref[...], wd_ref[...])).astype(bf16)
    for k in range(SUB - 1):
        for c in range(CAP):
            rows[k * owners : (k + 1) * owners, c * piece : (c + 1) * piece] = whole[
                c * owners : (c + 1) * owners, k * piece : (k + 1) * piece
            ]
    rows[(SUB - 1) * owners :, :lat] = jnp.broadcast_to(attn_ref[0:1, :], (owners, lat))
    rows[(SUB - 1) * owners :, lat:] = jnp.zeros((owners, width - lat), bf16)
    row, col = iota((total_rows, total_rows), 0), iota((total_rows, total_rows), 1)
    order = ones_where(col == (row % SUB) * owners + row // SUB)
    out_ref[...] = dot(order, rows[...]).astype(bf16)


def sum_kernel(len_ref, back_ref, ids_ref, gate_ref, moe_ref, attn_ref):
    total_rows, width = back_ref.shape
    owners = total_rows // SUB
    piece = width // CAP
    tok = ids_ref.shape[1]
    block = SUB * tok
    repeat, picks, match, rank = routing(ids_ref[...], owners, tok, len_ref[0])
    gates = gate_ref[...]
    lower = gates % 8
    split = []
    for number in (gates - lower, lower):
        number = dot(number.astype(f32).astype(bf16), repeat)
        split.append(sum(jnp.where(p, number[k : k + 1, :], 0.0) for k, p in enumerate(picks)))
    spread = ones_where(iota((owners, total_rows), 1) // SUB == iota((owners, total_rows), 0))
    row, col = iota((block, total_rows), 0), iota((block, total_rows), 1)
    kept = row // tok == col % SUB
    summed = jnp.zeros((block, piece), f32)
    for c in range(CAP):
        for number in split:
            mine = jnp.where((rank == c) & (match > 0.0), number, 0.0)
            lhs = dot(mine.T.astype(bf16), spread)
            lhs = jnp.where(kept, lhs, 0.0).astype(bf16)
            summed = summed + dot(lhs, back_ref[:, c * piece : (c + 1) * piece])
    summed = summed * (1.0 / gate_denominator)
    for k in range(SUB - 1):
        moe_ref[:, k * piece : (k + 1) * piece] = summed[k * tok : (k + 1) * tok].astype(bf16)
    lat = attn_ref.shape[1]
    last = ones_where(
        iota((owners, total_rows), 1) == iota((owners, total_rows), 0) * SUB + (SUB - 1)
    )
    attn_ref[...] = dot(last, back_ref[:, :lat]).astype(bf16)


def vmem():
    return pl.BlockSpec(memory_space=pltpu.VMEM)


def smem():
    return pl.BlockSpec(memory_space=pltpu.SMEM)


def hbm():
    return pl.BlockSpec(memory_space=pltpu.HBM)


def in_hbm(*arrays):
    return [pltpu.with_memory_space_constraint(a, pltpu.HBM) for a in arrays]


def in_vmem(*arrays):
    return [pltpu.with_memory_space_constraint(a, pltpu.VMEM) for a in arrays]


def call(kernel, out_shape, in_specs, scratch=(), vmem_mib=32):
    several = isinstance(out_shape, (tuple, list))
    return pl.pallas_call(
        kernel,
        out_shape=out_shape,
        in_specs=in_specs,
        out_specs=tuple(vmem() for _ in out_shape) if several else vmem(),
        scratch_shapes=list(scratch),
        compiler_params=pltpu.CompilerParams(vmem_limit_bytes=vmem_mib << 20),
        interpret=INTERPRET,
    )


def local(
    hidden_in,
    batch_len,
    expert_ids,
    gate_num,
    w_gate,
    w_up,
    w_down,
    q_latent,
    q_rope,
    kv_latent,
    kv_rope,
    ctx_len,
):
    owners = lax.axis_size("expert")
    tok, features = hidden_in.shape
    half = features // 2
    hidden_units = w_gate.shape[2]
    batch, heads, lat = q_latent.shape
    total_rows = owners * SUB
    slots = CAP * owners
    width = CAP * half // (SUB - 1)
    tensor = lax.axis_index("tensor")
    swap = [(0, 1), (1, 0)]

    def exchanged(packed):
        whole = packed.reshape(owners, SUB, width)
        return lax.all_to_all(whole, "expert", 0, 0, tiled=True).reshape(total_rows, width)

    ids_t, gate_t = expert_ids.T, gate_num.T
    local_arrays = (hidden_in, ids_t, q_latent, q_rope, kv_latent, kv_rope)
    packed = call(
        pack_kernel,
        jax.ShapeDtypeStruct((total_rows, width), bf16),
        [smem(), smem()] + [hbm() for _ in local_arrays],
        [pltpu.VMEM(a.shape, a.dtype) for a in local_arrays]
        + [pltpu.SemaphoreType.DMA((len(local_arrays),))],
    )(batch_len, ctx_len, *in_hbm(*local_arrays))
    own = exchanged(packed)
    given = lax.dynamic_slice_in_dim(w_down[0], (1 - tensor) * half, half, 1)
    down_other = lax.ppermute(given, "tensor", swap)
    other = lax.ppermute(own, "tensor", swap)
    partial = jax.ShapeDtypeStruct((slots, hidden_units), f32)
    half_weights = pltpu.VMEM((half, hidden_units), bf16)
    gate, upper, attn, next_gate, next_up = call(
        own_kernel,
        (partial, partial, jax.ShapeDtypeStruct((16, lat), bf16), half_weights, half_weights),
        [vmem(), hbm(), hbm()],
        [
            half_weights,
            half_weights,
            pltpu.VMEM((slots, half), bf16),
            pltpu.SemaphoreType.DMA((4,)),
        ],
    )(own, *in_hbm(w_gate, w_up))
    hidden, next_down = call(
        other_kernel,
        (
            jax.ShapeDtypeStruct((slots, hidden_units), bf16),
            pltpu.VMEM((hidden_units, half), bf16),
        ),
        [vmem() for _ in range(5)] + [hbm()],
        [pltpu.VMEM((slots, half), bf16), pltpu.SemaphoreType.DMA((1,))],
    )(other, *in_vmem(next_gate, next_up), gate, upper, *in_hbm(w_down))
    hidden_other = lax.ppermute(hidden, "tensor", swap)
    summed = call(down_kernel, jax.ShapeDtypeStruct((slots, half), f32), [vmem(), vmem()])(
        hidden, *in_vmem(next_down)
    )
    returned = call(
        back_kernel,
        jax.ShapeDtypeStruct((total_rows, width), bf16),
        [vmem() for _ in range(4)],
        [pltpu.VMEM((total_rows, width), bf16)],
    )(summed, hidden_other, down_other, attn)
    back = exchanged(returned)
    moe_half, attn_out = call(
        sum_kernel,
        (
            jax.ShapeDtypeStruct((tok, half), bf16),
            jax.ShapeDtypeStruct((batch * heads, lat), bf16),
        ),
        [smem(), vmem(), vmem(), vmem()],
    )(batch_len, back, ids_t, gate_t)
    moe_other = lax.ppermute(moe_half, "tensor", swap)
    moe_out = jnp.where(
        tensor == 0,
        jnp.concatenate([moe_half, moe_other], axis=1),
        jnp.concatenate([moe_other, moe_half], axis=1),
    )
    return moe_out, attn_out.reshape(batch, heads, lat)


def solution(mesh):
    both = ("groups", "expert")
    in_specs = (
        P(both, None),
        P("groups"),
        P(both, None),
        P(both, None),
        P("expert", None, "tensor"),
        P("expert", None, "tensor"),
        P("expert", "tensor", None),
        P("groups", "tensor", None),
        P("groups", "tensor", None),
        P("groups", "expert", None),
        P("groups", None, "expert"),
        P("groups"),
    )
    out_specs = (P(both, None), P("groups", "tensor", None))
    return jax.shard_map(local, mesh=mesh, in_specs=in_specs, out_specs=out_specs, check_vma=False)
```

```python
import jax
import jax.numpy as jnp
from jax import lax
from jax.experimental import pallas as pl
from jax.experimental.pallas import tpu as pltpu
from jax.sharding import PartitionSpec as P

SUB = 8
CAP = 3
bf16 = jnp.bfloat16
f32 = jnp.float32
softmax_scale = 192.0 ** (-0.5)
gate_denominator = 1024.0
BLOCKS = 2


def iota(shape, dim):
    return lax.broadcasted_iota(jnp.int32, shape, dim)


def dot(a, b):
    return jnp.dot(a, b, preferred_element_type=f32)


def dot_nt(a, b):
    return lax.dot_general(a, b, (((1,), (1,)), ((), ())), preferred_element_type=f32)


def ones_where(condition, dtype=bf16):
    return jnp.where(condition, 1.0, 0.0).astype(dtype)


def in_three(value):
    high = value.astype(bf16).astype(f32)
    middle = (value - high).astype(bf16).astype(f32)
    return high, middle, (value - high - middle).astype(bf16).astype(f32)


def routing(ids_t, owners, tok, live_count):
    topk = ids_t.shape[0]
    lanes = SUB * tok
    repeat = ones_where(iota((tok, lanes), 1) % tok == iota((tok, lanes), 0))
    ids = dot(ids_t.astype(f32).astype(bf16), repeat)
    row = iota((owners, lanes), 0).astype(f32)
    picks = [ids[k : k + 1, :] == row for k in range(topk)]
    live = lax.axis_index("expert") * tok + iota((owners, lanes), 1) % tok < live_count
    match = sum(ones_where(p, f32) for p in picks)
    match = jnp.where(live, match, 0.0)
    first, second = iota((lanes, lanes), 0), iota((lanes, lanes), 1)
    before = ones_where((first // tok == second // tok) & (first < second))
    return repeat, picks, match, dot(match.astype(bf16), before)


def pack_kernel(
    len_ref, ctx_hbm, hid_hbm, ids_hbm, ql_hbm, qr_hbm, kl_hbm, kr_hbm,
    out_ref,
    ctx_ref, hid_ref, ids_ref, ql_ref, qr_ref, kl_ref, kr_ref, sems,
):
    pairs = (
        (ql_hbm, ql_ref), (kl_hbm, kl_ref), (qr_hbm, qr_ref), (kr_hbm, kr_ref), (ctx_hbm, ctx_ref),
        (ids_hbm, ids_ref), (hid_hbm, hid_ref),
    )
    copies = copied(pairs, sems)
    expert, tensor = lax.axis_index("expert"), lax.axis_index("tensor")
    total_rows, width = out_ref.shape
    owners = total_rows // SUB
    piece = width // CAP
    tok = hid_ref.shape[0]
    half = hid_ref.shape[1] // 2
    batch, heads, lat = ql_ref.shape
    ctx_dev = kl_ref.shape[1]

    block = SUB * tok
    row, col = iota((total_rows, block), 0), iota((total_rows, block), 1)
    kept = (row % SUB == col // tok) & (col < block - tok)
    spread = ones_where(iota((total_rows, owners), 0) // SUB == iota((total_rows, owners), 1))
    last = ones_where(
        iota((total_rows, owners), 0) == iota((total_rows, owners), 1) * SUB + (SUB - 1)
    )
    for copy in copies[:5]:
        copy.wait()
    parts = []
    for b in range(batch):
        latent = kl_ref[b]
        s = dot_nt(ql_ref[b], latent) + dot(qr_ref[b], kr_ref[b])
        valid = expert * ctx_dev + iota((heads, ctx_dev), 1) < ctx_ref[b]
        s = jnp.where(valid, s * softmax_scale, -1e30)
        top = jnp.max(s, axis=1, keepdims=True)
        p = jnp.where(valid, jnp.exp(s - top), 0.0)
        total = jnp.sum(p, axis=1, keepdims=True)
        mean = dot(p.astype(bf16), latent) / jnp.where(total > 0.0, total, 1.0)
        at = iota((heads, width - lat), 1)
        stats = jnp.zeros((heads, width - lat), f32)
        for k, number in enumerate(in_three(top) + in_three(total)):
            stats = jnp.where(at == k, number, stats)
        parts.append(jnp.concatenate([mean, stats], axis=1).astype(bf16))
    attn = jnp.concatenate(parts, axis=0)

    for copy in copies[5:]:
        copy.wait()
    _, _, match, rank = routing(ids_ref[...], owners, tok, len_ref[0])
    hidden = hid_ref[...]
    source = jnp.where(tensor == 0, hidden[:, :half], hidden[:, half:])
    stacked = [source[:, k * piece : (k + 1) * piece] for k in range(half // piece)]
    stacked.append(jnp.zeros((tok, piece), bf16))
    stacked = jnp.concatenate(stacked, axis=0)
    for c in range(CAP):
        mine = jnp.where(rank == c, match, 0.0).astype(bf16)
        lhs = jnp.where(kept, dot(spread, mine), 0.0).astype(bf16)
        at = slice(c * piece, (c + 1) * piece)
        out_ref[:, at] = (dot(lhs, stacked) + dot(last, attn[:, at])).astype(bf16)


def sort_rows(arrived, rows):
    total_rows, width = arrived.shape
    owners = total_rows // SUB
    piece = width // CAP
    part = owners // BLOCKS
    size = SUB * part
    row, col = iota((size, size), 0), iota((size, size), 1)
    order = ones_where(col == (row % part) * SUB + row // part)
    attention = []
    for b in range(BLOCKS):
        ordered = dot(order, arrived[b * size : (b + 1) * size])
        for k in range(SUB - 1):
            for c in range(CAP):
                first = c * owners + b * part
                rows[first : first + part, k * piece : (k + 1) * piece] = ordered[
                    k * part : (k + 1) * part, c * piece : (c + 1) * piece
                ].astype(bf16)
        attention.append(ordered[size - part :])
    return jnp.concatenate(attention, axis=0)


def copied(pairs, sems):
    copies = [pltpu.make_async_copy(a, b, sems.at[k]) for k, (a, b) in enumerate(pairs)]
    for copy in copies:
        copy.start()
    return copies


def own_kernel(
    own_ref, wg_hbm, wu_hbm,
    gate_ref, upper_ref, attn_ref, next_gate_ref, next_up_ref,
    wg, wu, rows, sems,
):
    half = rows.shape[1]
    lat = attn_ref.shape[1]
    tensor = lax.axis_index("tensor")
    mine = pl.ds(pl.multiple_of(tensor * half, half), half)
    theirs = pl.ds(pl.multiple_of((1 - tensor) * half, half), half)
    copies = copied(
        (
            (wg_hbm.at[0, mine, :], wg),
            (wu_hbm.at[0, mine, :], wu),
            (wg_hbm.at[0, theirs, :], next_gate_ref),
            (wu_hbm.at[0, theirs, :], next_up_ref),
        ),
        sems,
    )
    arrived = sort_rows(own_ref[...], rows)
    stats = [arrived[:, lat + k : lat + k + 1] for k in range(6)]
    top = stats[0] + stats[1] + stats[2]
    total = stats[3] + stats[4] + stats[5]
    share = jnp.exp(top - jnp.max(top, axis=0, keepdims=True)) * total
    weighted = jnp.sum(share * arrived[:, :lat], axis=0, keepdims=True)
    done = weighted / jnp.sum(share, axis=0, keepdims=True)
    attn_ref[...] = jnp.broadcast_to(done, attn_ref.shape).astype(bf16)
    copies[0].wait()
    gate_ref[...] = dot(rows[...], wg[...])
    copies[1].wait()
    upper_ref[...] = dot(rows[...], wu[...])
    copies[2].wait()
    copies[3].wait()


def other_kernel(
    other_ref, wg_ref, wu_ref, gate_ref, upper_ref, wd_hbm,
    hidden_ref, next_down_ref,
    rows, sems,
):
    half = rows.shape[1]
    mine = pl.ds(pl.multiple_of(lax.axis_index("tensor") * half, half), half)
    copies = copied(((wd_hbm.at[0, :, mine], next_down_ref),), sems)
    sort_rows(other_ref[...], rows)
    gate = gate_ref[...] + dot(rows[...], wg_ref[...])
    upper = upper_ref[...] + dot(rows[...], wu_ref[...])
    hidden_ref[...] = (gate / (1.0 + jnp.exp(-gate)) * upper).astype(bf16)
    copies[0].wait()


def down_kernel(hidden_ref, wd_ref, len_ref, ids_ref, gate_ref, sum_ref, weigh_ref):
    sum_ref[...] = dot(hidden_ref[...], wd_ref[...])
    weigh(len_ref, ids_ref, gate_ref, weigh_ref)


def back_kernel(sum_ref, hidden_ref, wd_ref, attn_ref, out_ref, rows):
    total_rows, width = out_ref.shape
    owners = total_rows // SUB
    piece = width // CAP
    lat = attn_ref.shape[1]
    mine = pl.ds(pl.multiple_of(lax.axis_index("tensor") * sum_ref.shape[1], sum_ref.shape[1]), sum_ref.shape[1])
    whole = (sum_ref[...] + dot(hidden_ref[...], wd_ref[0, :, mine])).astype(bf16)
    part = owners // BLOCKS
    size = SUB * part
    row, col = iota((size, size), 0), iota((size, size), 1)
    order = ones_where(col == (row % SUB) * part + row // SUB)
    rows[size - part :, :lat] = jnp.broadcast_to(attn_ref[0:1, :], (part, lat))
    rows[size - part :, lat:] = jnp.zeros((part, width - lat), bf16)
    for b in range(BLOCKS):
        for k in range(SUB - 1):
            for c in range(CAP):
                first = c * owners + b * part
                rows[k * part : (k + 1) * part, c * piece : (c + 1) * piece] = whole[
                    first : first + part, k * piece : (k + 1) * piece
                ]
        out_ref[b * size : (b + 1) * size, :] = dot(order, rows[...]).astype(bf16)


def weigh(len_ref, ids_ref, gate_ref, weigh_ref):
    tok = ids_ref.shape[1]
    block, total_rows = SUB * tok, weigh_ref.shape[2]
    owners = total_rows // SUB
    repeat, picks, match, rank = routing(ids_ref[...], owners, tok, len_ref[0])
    gates = gate_ref[...]
    lower = gates % 8
    split = []
    for number in (gates - lower, lower):
        number = dot(number.astype(f32).astype(bf16), repeat)
        split.append(sum(jnp.where(p, number[k : k + 1, :], 0.0) for k, p in enumerate(picks)))
    spread = ones_where(iota((owners, total_rows), 1) // SUB == iota((owners, total_rows), 0))
    row, col = iota((block, total_rows), 0), iota((block, total_rows), 1)
    kept = row // tok == col % SUB
    for c in range(CAP):
        for n, number in enumerate(split):
            mine = jnp.where((rank == c) & (match > 0.0), number, 0.0)
            weigh_ref[2 * c + n] = jnp.where(kept, dot(mine.T.astype(bf16), spread), 0.0).astype(bf16)


def sum_kernel(weigh_ref, back_ref, moe_ref, attn_ref):
    total_rows, width = back_ref.shape
    owners = total_rows // SUB
    piece = width // CAP
    tok, _ = moe_ref.shape
    summed = sum(
        dot(weigh_ref[2 * c + n], back_ref[:, c * piece : (c + 1) * piece])
        for c in range(CAP)
        for n in range(2)
    ) * (1.0 / gate_denominator)
    for k in range(SUB - 1):
        moe_ref[:, k * piece : (k + 1) * piece] = summed[k * tok : (k + 1) * tok].astype(bf16)
    lat = attn_ref.shape[1]
    last = ones_where(
        iota((owners, total_rows), 1) == iota((owners, total_rows), 0) * SUB + (SUB - 1)
    )
    attn_ref[...] = dot(last, back_ref[:, :lat]).astype(bf16)


def vmem():
    return pl.BlockSpec(memory_space=pltpu.VMEM)


def smem():
    return pl.BlockSpec(memory_space=pltpu.SMEM)


def hbm():
    return pl.BlockSpec(memory_space=pltpu.HBM)


def in_hbm(*arrays):
    return [pltpu.with_memory_space_constraint(a, pltpu.HBM) for a in arrays]


def in_vmem(*arrays):
    return [pltpu.with_memory_space_constraint(a, pltpu.VMEM) for a in arrays]


def call(kernel, out_shape, in_specs, scratch=(), vmem_mib=32):
    several = isinstance(out_shape, (tuple, list))
    return pl.pallas_call(
        kernel,
        out_shape=out_shape,
        in_specs=in_specs,
        out_specs=tuple(vmem() for _ in out_shape) if several else vmem(),
        scratch_shapes=list(scratch),
        compiler_params=pltpu.CompilerParams(vmem_limit_bytes=vmem_mib << 20),
    )


def local(
    hidden_in,
    batch_len,
    expert_ids,
    gate_num,
    w_gate,
    w_up,
    w_down,
    q_latent,
    q_rope,
    kv_latent,
    kv_rope,
    ctx_len,
):
    owners = lax.axis_size("expert")
    tok, features = hidden_in.shape
    half = features // 2
    hidden_units = w_gate.shape[2]
    batch, heads, lat = q_latent.shape
    total_rows = owners * SUB
    slots = CAP * owners
    width = CAP * half // (SUB - 1)
    tensor = lax.axis_index("tensor")
    swap = [(0, 1), (1, 0)]

    def exchanged(packed):
        whole = packed.reshape(owners, SUB, width)
        return lax.all_to_all(whole, "expert", 0, 0, tiled=True).reshape(total_rows, width)

    ids_t, gate_t = expert_ids.T, gate_num.T
    arrays = (hidden_in, ids_t, q_latent, q_rope, kv_latent, kv_rope)
    packed = call(
        pack_kernel,
        pltpu.VMEM((total_rows, width), bf16),
        [smem()] + [hbm() for _ in range(7)],
        [pltpu.SMEM(ctx_len.shape, ctx_len.dtype)]
        + [pltpu.VMEM(a.shape, a.dtype) for a in arrays]
        + [pltpu.SemaphoreType.DMA((7,))],
    )(batch_len, *in_hbm(ctx_len, *arrays))
    own = exchanged(packed)
    other = lax.ppermute(own, "tensor", swap)
    down_other = lax.ppermute(w_down, "tensor", swap)
    partial = jax.ShapeDtypeStruct((slots, hidden_units), f32)
    half_weights = pltpu.VMEM((half, hidden_units), bf16)
    gate, upper, attn, next_gate, next_up = call(
        own_kernel,
        (partial, partial, jax.ShapeDtypeStruct((16, lat), bf16), half_weights, half_weights),
        [vmem(), hbm(), hbm()],
        [
            half_weights,
            half_weights,
            pltpu.VMEM((slots, half), bf16),
            pltpu.SemaphoreType.DMA((4,)),
        ],
    )(own, *in_hbm(w_gate, w_up))
    hidden, next_down = call(
        other_kernel,
        (
            jax.ShapeDtypeStruct((slots, hidden_units), bf16),
            pltpu.VMEM((hidden_units, half), bf16),
        ),
        [vmem() for _ in range(5)] + [hbm()],
        [pltpu.VMEM((slots, half), bf16), pltpu.SemaphoreType.DMA((1,))],
    )(other, *in_vmem(next_gate, next_up), gate, upper, *in_hbm(w_down))
    hidden_other = lax.ppermute(hidden, "tensor", swap)
    summed, weights = call(
        down_kernel,
        (
            jax.ShapeDtypeStruct((slots, half), f32),
            jax.ShapeDtypeStruct((2 * CAP, SUB * tok, total_rows), bf16),
        ),
        [vmem(), vmem(), smem(), vmem(), vmem()],
    )(hidden, *in_vmem(next_down), batch_len, ids_t, gate_t)
    returned = call(
        back_kernel,
        jax.ShapeDtypeStruct((total_rows, width), bf16),
        [vmem() for _ in range(4)],
        [pltpu.VMEM((total_rows // BLOCKS, width), bf16)],
    )(summed, hidden_other, *in_vmem(down_other), attn)
    back = exchanged(returned)
    moe_half, attn_out = call(
        sum_kernel,
        (
            jax.ShapeDtypeStruct((tok, half), bf16),
            jax.ShapeDtypeStruct((batch * heads, lat), bf16),
        ),
        [vmem(), vmem()],
    )(weights, back)
    moe_other = lax.ppermute(moe_half, "tensor", swap)
    moe_out = jnp.where(
        tensor == 0,
        jnp.concatenate([moe_half, moe_other], axis=1),
        jnp.concatenate([moe_other, moe_half], axis=1),
    )
    return moe_out, attn_out.reshape(batch, heads, lat)


def solution(mesh):
    both = ("groups", "expert")
    in_specs = (
        P(both, None),
        P("groups"),
        P(both, None),
        P(both, None),
        P("expert", None, "tensor"),
        P("expert", None, "tensor"),
        P("expert", "tensor", None),
        P("groups", "tensor", None),
        P("groups", "tensor", None),
        P("groups", "expert", None),
        P("groups", None, "expert"),
        P("groups"),
    )
    out_specs = (P(both, None), P("groups", "tensor", None))
    return jax.shard_map(local, mesh=mesh, in_specs=in_specs, out_specs=out_specs, check_vma=False)
```

```python
import jax
import jax.numpy as jnp
from jax import lax
from jax.experimental import pallas as pl
from jax.experimental.pallas import tpu as pltpu
from jax.sharding import PartitionSpec as P

SUB = 8
CAP = 3
bf16 = jnp.bfloat16
f32 = jnp.float32
softmax_scale = 192.0 ** (-0.5)
gate_denominator = 1024.0
BLOCKS = 2


def iota(shape, dim):
    return lax.broadcasted_iota(jnp.int32, shape, dim)


def dot(a, b):
    return jnp.dot(a, b, preferred_element_type=f32)


def dot_nt(a, b):
    return lax.dot_general(a, b, (((1,), (1,)), ((), ())), preferred_element_type=f32)


def ones_where(condition, dtype=bf16):
    return jnp.where(condition, 1.0, 0.0).astype(dtype)


def in_three(value):
    high = value.astype(bf16).astype(f32)
    middle = (value - high).astype(bf16).astype(f32)
    return high, middle, (value - high - middle).astype(bf16).astype(f32)


def routing(ids_t, owners, tok, live_count):
    topk = ids_t.shape[0]
    lanes = SUB * tok
    repeat = ones_where(iota((tok, lanes), 1) % tok == iota((tok, lanes), 0))
    ids = dot(ids_t.astype(f32).astype(bf16), repeat)
    row = iota((owners, lanes), 0).astype(f32)
    picks = [ids[k : k + 1, :] == row for k in range(topk)]
    live = lax.axis_index("expert") * tok + iota((owners, lanes), 1) % tok < live_count
    match = sum(ones_where(p, f32) for p in picks)
    match = jnp.where(live, match, 0.0)
    first, second = iota((lanes, lanes), 0), iota((lanes, lanes), 1)
    before = ones_where((first // tok == second // tok) & (first < second))
    return repeat, picks, match, dot(match.astype(bf16), before)


def pack_kernel(
    len_ref, ctx_hbm, hid_hbm, ids_hbm, ql_hbm, qr_hbm, kl_hbm, kr_hbm, wg_hbm, wd_hbm,
    out_ref, first_gate_ref, give_ref,
    ctx_ref, hid_ref, ids_ref, ql_ref, qr_ref, kl_ref, kr_ref, sems,
):
    expert, tensor = lax.axis_index("expert"), lax.axis_index("tensor")
    half = hid_ref.shape[1] // 2
    mine = pl.ds(pl.multiple_of(tensor * half, half), half)
    theirs = pl.ds(pl.multiple_of((1 - tensor) * half, half), half)
    copies = copied(
        (
            (ql_hbm, ql_ref), (kl_hbm, kl_ref), (qr_hbm, qr_ref), (kr_hbm, kr_ref),
            (ctx_hbm, ctx_ref), (ids_hbm, ids_ref), (hid_hbm, hid_ref),
            (wd_hbm.at[0, :, theirs], give_ref), (wg_hbm.at[0, mine, :], first_gate_ref),
        ),
        sems,
    )
    total_rows, width = out_ref.shape
    owners = total_rows // SUB
    piece = width // CAP
    tok = hid_ref.shape[0]
    batch, heads, lat = ql_ref.shape
    ctx_dev = kl_ref.shape[1]

    block = SUB * tok
    sub, lane = iota((SUB, block), 0), iota((SUB, block), 1)
    kept = (sub == lane // tok) & (lane < block - tok)
    last = ones_where(
        iota((total_rows, owners), 0) == iota((total_rows, owners), 1) * SUB + (SUB - 1)
    )
    for copy in copies[:7]:
        copy.wait()
    parts = []
    for b in range(batch):
        latent = kl_ref[b]
        s = dot_nt(ql_ref[b], latent) + dot(qr_ref[b], kr_ref[b])
        valid = expert * ctx_dev + iota((heads, ctx_dev), 1) < ctx_ref[b]
        s = jnp.where(valid, s * softmax_scale, -1e30)
        top = jnp.max(s, axis=1, keepdims=True)
        p = jnp.where(valid, jnp.exp(s - top), 0.0)
        total = jnp.sum(p, axis=1, keepdims=True)
        mean = dot(p.astype(bf16), latent) / jnp.where(total > 0.0, total, 1.0)
        at = iota((heads, width - lat), 1)
        stats = jnp.zeros((heads, width - lat), f32)
        for k, number in enumerate(in_three(top) + in_three(total)):
            stats = jnp.where(at == k, number, stats)
        parts.append(jnp.concatenate([mean, stats], axis=1).astype(bf16))
    attn = jnp.concatenate(parts, axis=0)

    _, _, match, rank = routing(ids_ref[...], owners, tok, len_ref[0])
    hidden = hid_ref[...]
    source = jnp.where(tensor == 0, hidden[:, :half], hidden[:, half:])
    stacked = [source[:, k * piece : (k + 1) * piece] for k in range(half // piece)]
    stacked.append(jnp.zeros((tok, piece), bf16))
    stacked = jnp.concatenate(stacked, axis=0)
    for c in range(CAP):
        mine = jnp.where(rank == c, match, 0.0)
        lhs = jnp.where(kept, mine[:, None, :], 0.0).reshape(total_rows, block).astype(bf16)
        at = slice(c * piece, (c + 1) * piece)
        lhs = jnp.concatenate([lhs, last], axis=1)
        rhs = jnp.concatenate([stacked, attn[:, at]], axis=0)
        out_ref[:, at] = dot(lhs, rhs).astype(bf16)
    for copy in copies[7:]:
        copy.wait()


def sort_rows(arrived, rows):
    total_rows, width = arrived.shape
    owners = total_rows // SUB
    piece = width // CAP
    part = owners // BLOCKS
    size = SUB * part
    row, col = iota((size, size), 0), iota((size, size), 1)
    order = ones_where(col == (row % part) * SUB + row // part)
    attention = []
    for b in range(BLOCKS):
        ordered = dot(order, arrived[b * size : (b + 1) * size])
        for k in range(SUB - 1):
            for c in range(CAP):
                first = c * owners + b * part
                rows[first : first + part, k * piece : (k + 1) * piece] = ordered[
                    k * part : (k + 1) * part, c * piece : (c + 1) * piece
                ].astype(bf16)
        attention.append(ordered[size - part :])
    return jnp.concatenate(attention, axis=0)


def copied(pairs, sems):
    copies = [pltpu.make_async_copy(a, b, sems.at[k]) for k, (a, b) in enumerate(pairs)]
    for copy in copies:
        copy.start()
    return copies


def own_kernel(
    own_ref, wg_ref, wg_hbm, wu_hbm,
    gate_ref, upper_ref, attn_ref, next_gate_ref, next_up_ref,
    wu, rows, sems,
):
    half = rows.shape[1]
    lat = attn_ref.shape[1]
    tensor = lax.axis_index("tensor")
    mine = pl.ds(pl.multiple_of(tensor * half, half), half)
    theirs = pl.ds(pl.multiple_of((1 - tensor) * half, half), half)
    copies = copied(
        (
            (wu_hbm.at[0, mine, :], wu),
            (wg_hbm.at[0, theirs, :], next_gate_ref),
            (wu_hbm.at[0, theirs, :], next_up_ref),
        ),
        sems,
    )
    arrived = sort_rows(own_ref[...], rows)
    stats = [arrived[:, lat + k : lat + k + 1] for k in range(6)]
    top = stats[0] + stats[1] + stats[2]
    total = stats[3] + stats[4] + stats[5]
    share = jnp.exp(top - jnp.max(top, axis=0, keepdims=True)) * total
    weighted = jnp.sum(share * arrived[:, :lat], axis=0, keepdims=True)
    done = weighted / jnp.sum(share, axis=0, keepdims=True)
    attn_ref[...] = jnp.broadcast_to(done, attn_ref.shape).astype(bf16)
    gate_ref[...] = dot(rows[...], wg_ref[...])
    copies[0].wait()
    upper_ref[...] = dot(rows[...], wu[...])
    copies[1].wait()
    copies[2].wait()


def other_kernel(
    other_ref, wg_ref, wu_ref, gate_ref, upper_ref, wd_hbm,
    hidden_ref, next_down_ref,
    rows, sems,
):
    half = rows.shape[1]
    mine = pl.ds(pl.multiple_of(lax.axis_index("tensor") * half, half), half)
    copies = copied(((wd_hbm.at[0, :, mine], next_down_ref),), sems)
    sort_rows(other_ref[...], rows)
    gate = gate_ref[...] + dot(rows[...], wg_ref[...])
    upper = upper_ref[...] + dot(rows[...], wu_ref[...])
    hidden_ref[...] = (gate / (1.0 + jnp.exp(-gate)) * upper).astype(bf16)
    copies[0].wait()


def down_kernel(hidden_ref, wd_ref, len_ref, ids_ref, gate_ref, sum_ref, weigh_ref):
    sum_ref[...] = dot(hidden_ref[...], wd_ref[...])
    weigh(len_ref, ids_ref, gate_ref, weigh_ref)


def back_kernel(sum_ref, hidden_ref, wd_ref, attn_ref, out_ref, rows):
    total_rows, width = out_ref.shape
    owners = total_rows // SUB
    piece = width // CAP
    lat = attn_ref.shape[1]
    whole = (sum_ref[...] + dot(hidden_ref[...], wd_ref[...])).astype(bf16)
    part = owners // BLOCKS
    size = SUB * part
    row, col = iota((size, size), 0), iota((size, size), 1)
    order = ones_where(col == (row % SUB) * part + row // SUB)
    rows[size - part :, :lat] = jnp.broadcast_to(attn_ref[0:1, :], (part, lat))
    rows[size - part :, lat:] = jnp.zeros((part, width - lat), bf16)
    for b in range(BLOCKS):
        for k in range(SUB - 1):
            for c in range(CAP):
                first = c * owners + b * part
                rows[k * part : (k + 1) * part, c * piece : (c + 1) * piece] = whole[
                    first : first + part, k * piece : (k + 1) * piece
                ]
        out_ref[b * size : (b + 1) * size, :] = dot(order, rows[...]).astype(bf16)


def weigh(len_ref, ids_ref, gate_ref, weigh_ref):
    tok = ids_ref.shape[1]
    block, total_rows = SUB * tok, weigh_ref.shape[2]
    owners = total_rows // SUB
    repeat, picks, match, rank = routing(ids_ref[...], owners, tok, len_ref[0])
    gates = gate_ref[...]
    lower = gates % 8
    split = []
    for number in (gates - lower, lower):
        number = dot(number.astype(f32).astype(bf16), repeat)
        split.append(sum(jnp.where(p, number[k : k + 1, :], 0.0) for k, p in enumerate(picks)))
    spread = ones_where(iota((owners, total_rows), 1) // SUB == iota((owners, total_rows), 0))
    row, col = iota((block, total_rows), 0), iota((block, total_rows), 1)
    kept = row // tok == col % SUB
    for c in range(CAP):
        for n, number in enumerate(split):
            mine = jnp.where((rank == c) & (match > 0.0), number, 0.0)
            weigh_ref[2 * c + n] = jnp.where(kept, dot(mine.T.astype(bf16), spread), 0.0).astype(bf16)


def sum_kernel(weigh_ref, back_ref, moe_ref, attn_ref):
    total_rows, width = back_ref.shape
    owners = total_rows // SUB
    piece = width // CAP
    tok, _ = moe_ref.shape
    summed = sum(
        dot(weigh_ref[2 * c + n], back_ref[:, c * piece : (c + 1) * piece])
        for c in range(CAP)
        for n in range(2)
    ) * (1.0 / gate_denominator)
    for k in range(SUB - 1):
        moe_ref[:, k * piece : (k + 1) * piece] = summed[k * tok : (k + 1) * tok].astype(bf16)
    lat = attn_ref.shape[1]
    last = ones_where(
        iota((owners, total_rows), 1) == iota((owners, total_rows), 0) * SUB + (SUB - 1)
    )
    attn_ref[...] = dot(last, back_ref[:, :lat]).astype(bf16)


def vmem():
    return pl.BlockSpec(memory_space=pltpu.VMEM)


def smem():
    return pl.BlockSpec(memory_space=pltpu.SMEM)


def hbm():
    return pl.BlockSpec(memory_space=pltpu.HBM)


def in_hbm(*arrays):
    return [pltpu.with_memory_space_constraint(a, pltpu.HBM) for a in arrays]


def in_vmem(*arrays):
    return [pltpu.with_memory_space_constraint(a, pltpu.VMEM) for a in arrays]


def call(kernel, out_shape, in_specs, scratch=(), vmem_mib=32):
    several = isinstance(out_shape, (tuple, list))
    return pl.pallas_call(
        kernel,
        out_shape=out_shape,
        in_specs=in_specs,
        out_specs=tuple(vmem() for _ in out_shape) if several else vmem(),
        scratch_shapes=list(scratch),
        compiler_params=pltpu.CompilerParams(vmem_limit_bytes=vmem_mib << 20),
    )


def local(
    hidden_in,
    batch_len,
    expert_ids,
    gate_num,
    w_gate,
    w_up,
    w_down,
    q_latent,
    q_rope,
    kv_latent,
    kv_rope,
    ctx_len,
):
    owners = lax.axis_size("expert")
    tok, features = hidden_in.shape
    half = features // 2
    hidden_units = w_gate.shape[2]
    batch, heads, lat = q_latent.shape
    total_rows = owners * SUB
    slots = CAP * owners
    width = CAP * half // (SUB - 1)
    tensor = lax.axis_index("tensor")
    swap = [(0, 1), (1, 0)]

    def exchanged(packed):
        whole = packed.reshape(owners, SUB, width)
        return lax.all_to_all(whole, "expert", 0, 0, tiled=True).reshape(total_rows, width)

    ids_t, gate_t = expert_ids.T, gate_num.T
    arrays = (hidden_in, ids_t, q_latent, q_rope, kv_latent, kv_rope)
    half_weights = pltpu.VMEM((half, hidden_units), bf16)
    half_down = pltpu.VMEM((hidden_units, half), bf16)
    packed, first_gate, given = call(
        pack_kernel,
        (pltpu.VMEM((total_rows, width), bf16), half_weights, half_down),
        [smem()] + [hbm() for _ in range(9)],
        [pltpu.SMEM(ctx_len.shape, ctx_len.dtype)]
        + [pltpu.VMEM(a.shape, a.dtype) for a in arrays]
        + [pltpu.SemaphoreType.DMA((9,))],
    )(batch_len, *in_hbm(ctx_len, *arrays, w_gate, w_down))
    own = exchanged(packed)
    other = lax.ppermute(own, "tensor", swap)
    down_other = lax.ppermute(given, "tensor", swap)
    partial = jax.ShapeDtypeStruct((slots, hidden_units), f32)
    gate, upper, attn, next_gate, next_up = call(
        own_kernel,
        (partial, partial, jax.ShapeDtypeStruct((16, lat), bf16), half_weights, half_weights),
        [vmem(), vmem(), hbm(), hbm()],
        [half_weights, pltpu.VMEM((slots, half), bf16), pltpu.SemaphoreType.DMA((3,))],
    )(own, *in_vmem(first_gate), *in_hbm(w_gate, w_up))
    hidden, next_down = call(
        other_kernel,
        (
            jax.ShapeDtypeStruct((slots, hidden_units), bf16),
            half_down,
        ),
        [vmem() for _ in range(5)] + [hbm()],
        [pltpu.VMEM((slots, half), bf16), pltpu.SemaphoreType.DMA((1,))],
    )(other, *in_vmem(next_gate, next_up), gate, upper, *in_hbm(w_down))
    hidden_other = lax.ppermute(hidden, "tensor", swap)
    summed, weights = call(
        down_kernel,
        (
            jax.ShapeDtypeStruct((slots, half), f32),
            jax.ShapeDtypeStruct((2 * CAP, SUB * tok, total_rows), bf16),
        ),
        [vmem(), vmem(), smem(), vmem(), vmem()],
    )(hidden, *in_vmem(next_down), batch_len, ids_t, gate_t)
    returned = call(
        back_kernel,
        jax.ShapeDtypeStruct((total_rows, width), bf16),
        [vmem() for _ in range(4)],
        [pltpu.VMEM((total_rows // BLOCKS, width), bf16)],
    )(summed, hidden_other, *in_vmem(down_other), attn)
    back = exchanged(returned)
    moe_half, attn_out = call(
        sum_kernel,
        (
            jax.ShapeDtypeStruct((tok, half), bf16),
            pltpu.VMEM((batch * heads, lat), bf16),
        ),
        [vmem(), vmem()],
    )(weights, back)
    moe_other = lax.ppermute(moe_half, "tensor", swap)
    moe_out = jnp.where(
        tensor == 0,
        jnp.concatenate([moe_half, moe_other], axis=1),
        jnp.concatenate([moe_other, moe_half], axis=1),
    )
    return moe_out, attn_out.reshape(batch, heads, lat)


def solution(mesh):
    both = ("groups", "expert")
    in_specs = (
        P(both, None),
        P("groups"),
        P(both, None),
        P(both, None),
        P("expert", None, "tensor"),
        P("expert", None, "tensor"),
        P("expert", "tensor", None),
        P("groups", "tensor", None),
        P("groups", "tensor", None),
        P("groups", "expert", None),
        P("groups", None, "expert"),
        P("groups"),
    )
    out_specs = (P(both, None), P("groups", "tensor", None))
    return jax.shard_map(local, mesh=mesh, in_specs=in_specs, out_specs=out_specs, check_vma=False)
```

```python
import jax
import jax.numpy as jnp
from jax import lax
from jax.experimental import pallas as pl
from jax.experimental.pallas import tpu as pltpu
from jax.sharding import PartitionSpec as P

SUB = 8
CAP = 3
bf16 = jnp.bfloat16
f32 = jnp.float32
softmax_scale = 192.0 ** (-0.5)
gate_denominator = 1024.0
BLOCKS = 2


def iota(shape, dim):
    return lax.broadcasted_iota(jnp.int32, shape, dim)


def dot(a, b):
    return jnp.dot(a, b, preferred_element_type=f32)


def dot_nt(a, b):
    return lax.dot_general(a, b, (((1,), (1,)), ((), ())), preferred_element_type=f32)


def ones_where(condition, dtype=bf16):
    return jnp.where(condition, 1.0, 0.0).astype(dtype)


def in_three(value):
    high = value.astype(bf16).astype(f32)
    middle = (value - high).astype(bf16).astype(f32)
    return high, middle, (value - high - middle).astype(bf16).astype(f32)


def routing(ids_t, owners, tok, live_count):
    topk = ids_t.shape[0]
    lanes = SUB * tok
    repeat = ones_where(iota((tok, lanes), 1) % tok == iota((tok, lanes), 0))
    ids = dot(ids_t.astype(f32).astype(bf16), repeat)
    row = iota((owners, lanes), 0).astype(f32)
    picks = [ids[k : k + 1, :] == row for k in range(topk)]
    live = lax.axis_index("expert") * tok + iota((owners, lanes), 1) % tok < live_count
    match = sum(ones_where(p, f32) for p in picks)
    match = jnp.where(live, match, 0.0)
    first, second = iota((lanes, lanes), 0), iota((lanes, lanes), 1)
    before = ones_where((first // tok == second // tok) & (first < second))
    return repeat, picks, match, dot(match.astype(bf16), before)


def pack_kernel(
    len_ref, ctx_hbm, hid_hbm, ids_hbm, ql_hbm, qr_hbm, kl_hbm, kr_hbm, wd_hbm,
    out_ref, give_ref,
    ctx_ref, hid_ref, ids_ref, ql_ref, qr_ref, kl_ref, kr_ref, sems,
):
    expert, tensor = lax.axis_index("expert"), lax.axis_index("tensor")
    half = hid_ref.shape[1] // 2
    mine = pl.ds(pl.multiple_of(tensor * half, half), half)
    theirs = pl.ds(pl.multiple_of((1 - tensor) * half, half), half)
    copies = copied(
        (
            (ql_hbm, ql_ref), (kl_hbm, kl_ref), (qr_hbm, qr_ref), (kr_hbm, kr_ref),
            (ctx_hbm, ctx_ref), (ids_hbm, ids_ref), (hid_hbm, hid_ref),
            (wd_hbm.at[0, :, theirs], give_ref),
        ),
        sems,
    )
    total_rows, width = out_ref.shape
    owners = total_rows // SUB
    piece = width // CAP
    tok = hid_ref.shape[0]
    batch, heads, lat = ql_ref.shape
    ctx_dev = kl_ref.shape[1]

    block = SUB * tok
    sub, lane = iota((SUB, block), 0), iota((SUB, block), 1)
    kept = (sub == lane // tok) & (lane < block - tok)
    last = ones_where(
        iota((total_rows, owners), 0) == iota((total_rows, owners), 1) * SUB + (SUB - 1)
    )
    for copy in copies[:7]:
        copy.wait()
    parts = []
    for b in range(batch):
        latent = kl_ref[b]
        s = dot_nt(ql_ref[b], latent) + dot(qr_ref[b], kr_ref[b])
        valid = expert * ctx_dev + iota((heads, ctx_dev), 1) < ctx_ref[b]
        s = jnp.where(valid, s * softmax_scale, -1e30)
        top = jnp.max(s, axis=1, keepdims=True)
        p = jnp.where(valid, jnp.exp(s - top), 0.0)
        total = jnp.sum(p, axis=1, keepdims=True)
        mean = dot(p.astype(bf16), latent) / jnp.where(total > 0.0, total, 1.0)
        at = iota((heads, width - lat), 1)
        stats = jnp.zeros((heads, width - lat), f32)
        for k, number in enumerate(in_three(top) + in_three(total)):
            stats = jnp.where(at == k, number, stats)
        parts.append(jnp.concatenate([mean, stats], axis=1).astype(bf16))
    attn = jnp.concatenate(parts, axis=0)

    _, _, match, rank = routing(ids_ref[...], owners, tok, len_ref[0])
    hidden = hid_ref[...]
    source = jnp.where(tensor == 0, hidden[:, :half], hidden[:, half:])
    stacked = [source[:, k * piece : (k + 1) * piece] for k in range(half // piece)]
    stacked.append(jnp.zeros((tok, piece), bf16))
    stacked = jnp.concatenate(stacked, axis=0)
    for c in range(CAP):
        mine = jnp.where(rank == c, match, 0.0)
        lhs = jnp.where(kept, mine[:, None, :], 0.0).reshape(total_rows, block).astype(bf16)
        at = slice(c * piece, (c + 1) * piece)
        lhs = jnp.concatenate([lhs, last], axis=1)
        rhs = jnp.concatenate([stacked, attn[:, at]], axis=0)
        out_ref[:, at] = dot(lhs, rhs).astype(bf16)
    for copy in copies[7:]:
        copy.wait()


def sort_rows(arrived, rows):
    total_rows, width = arrived.shape
    owners = total_rows // SUB
    piece = width // CAP
    part = owners // BLOCKS
    size = SUB * part
    row, col = iota((size, size), 0), iota((size, size), 1)
    order = ones_where(col == (row % part) * SUB + row // part)
    attention = []
    for b in range(BLOCKS):
        ordered = dot(order, arrived[b * size : (b + 1) * size])
        for k in range(SUB - 1):
            for c in range(CAP):
                first = c * owners + b * part
                rows[first : first + part, k * piece : (k + 1) * piece] = ordered[
                    k * part : (k + 1) * part, c * piece : (c + 1) * piece
                ].astype(bf16)
        attention.append(ordered[size - part :])
    return jnp.concatenate(attention, axis=0)


def copied(pairs, sems):
    copies = [pltpu.make_async_copy(a, b, sems.at[k]) for k, (a, b) in enumerate(pairs)]
    for copy in copies:
        copy.start()
    return copies


def own_kernel(
    own_ref, wg_ref, wu_hbm,
    gate_ref, upper_ref, attn_ref, next_up_ref,
    wu, rows, sems,
):
    half = rows.shape[1]
    lat = attn_ref.shape[1]
    tensor = lax.axis_index("tensor")
    mine = pl.ds(pl.multiple_of(tensor * half, half), half)
    theirs = pl.ds(pl.multiple_of((1 - tensor) * half, half), half)
    copies = copied(((wu_hbm.at[0, mine, :], wu), (wu_hbm.at[0, theirs, :], next_up_ref)), sems)
    arrived = sort_rows(own_ref[...], rows)
    stats = [arrived[:, lat + k : lat + k + 1] for k in range(6)]
    top = stats[0] + stats[1] + stats[2]
    total = stats[3] + stats[4] + stats[5]
    share = jnp.exp(top - jnp.max(top, axis=0, keepdims=True)) * total
    weighted = jnp.sum(share * arrived[:, :lat], axis=0, keepdims=True)
    done = weighted / jnp.sum(share, axis=0, keepdims=True)
    attn_ref[...] = jnp.broadcast_to(done, attn_ref.shape).astype(bf16)
    gate_ref[...] = dot(rows[...], wg_ref[0, mine, :])
    copies[0].wait()
    upper_ref[...] = dot(rows[...], wu[...])
    copies[1].wait()


def other_kernel(other_ref, wg_ref, wu_ref, gate_ref, upper_ref, hidden_ref, rows):
    half = rows.shape[1]
    theirs = pl.ds(pl.multiple_of((1 - lax.axis_index("tensor")) * half, half), half)
    sort_rows(other_ref[...], rows)
    gate = gate_ref[...] + dot(rows[...], wg_ref[0, theirs, :])
    upper = upper_ref[...] + dot(rows[...], wu_ref[...])
    hidden_ref[...] = (gate / (1.0 + jnp.exp(-gate)) * upper).astype(bf16)


def weigh_kernel(hidden_ref, len_ref, ids_ref, gate_ref, weigh_ref):
    weigh(len_ref, ids_ref, gate_ref, weigh_ref)


def down_kernel(hidden_ref, wd_ref, weigh_ref, sum_ref):
    half = sum_ref.shape[1]
    mine = pl.ds(pl.multiple_of(lax.axis_index("tensor") * half, half), half)
    sum_ref[...] = dot(hidden_ref[...], wd_ref[0, :, mine])


def back_kernel(sum_ref, hidden_ref, wd_ref, attn_ref, out_ref, rows):
    total_rows, width = out_ref.shape
    owners = total_rows // SUB
    piece = width // CAP
    lat = attn_ref.shape[1]
    whole = (sum_ref[...] + dot(hidden_ref[...], wd_ref[...])).astype(bf16)
    part = owners // BLOCKS
    size = SUB * part
    row, col = iota((size, size), 0), iota((size, size), 1)
    order = ones_where(col == (row % SUB) * part + row // SUB)
    rows[size - part :, :lat] = jnp.broadcast_to(attn_ref[0:1, :], (part, lat))
    rows[size - part :, lat:] = jnp.zeros((part, width - lat), bf16)
    for b in range(BLOCKS):
        for k in range(SUB - 1):
            for c in range(CAP):
                first = c * owners + b * part
                rows[k * part : (k + 1) * part, c * piece : (c + 1) * piece] = whole[
                    first : first + part, k * piece : (k + 1) * piece
                ]
        out_ref[b * size : (b + 1) * size, :] = dot(order, rows[...]).astype(bf16)


def weigh(len_ref, ids_ref, gate_ref, weigh_ref):
    tok = ids_ref.shape[1]
    block, total_rows = SUB * tok, weigh_ref.shape[2]
    owners = total_rows // SUB
    repeat, picks, match, rank = routing(ids_ref[...], owners, tok, len_ref[0])
    gates = gate_ref[...]
    lower = gates % 8
    split = []
    for number in (gates - lower, lower):
        number = dot(number.astype(f32).astype(bf16), repeat)
        split.append(sum(jnp.where(p, number[k : k + 1, :], 0.0) for k, p in enumerate(picks)))
    spread = ones_where(iota((owners, total_rows), 1) // SUB == iota((owners, total_rows), 0))
    row, col = iota((block, total_rows), 0), iota((block, total_rows), 1)
    kept = row // tok == col % SUB
    for c in range(CAP):
        for n, number in enumerate(split):
            mine = jnp.where((rank == c) & (match > 0.0), number, 0.0)
            weigh_ref[2 * c + n] = jnp.where(kept, dot(mine.T.astype(bf16), spread), 0.0).astype(bf16)


def sum_kernel(weigh_ref, back_ref, moe_ref, attn_ref):
    total_rows, width = back_ref.shape
    owners = total_rows // SUB
    piece = width // CAP
    tok, _ = moe_ref.shape
    summed = sum(
        dot(weigh_ref[2 * c + n], back_ref[:, c * piece : (c + 1) * piece])
        for c in range(CAP)
        for n in range(2)
    ) * (1.0 / gate_denominator)
    for k in range(SUB - 1):
        moe_ref[:, k * piece : (k + 1) * piece] = summed[k * tok : (k + 1) * tok].astype(bf16)
    lat = attn_ref.shape[1]
    last = ones_where(
        iota((owners, total_rows), 1) == iota((owners, total_rows), 0) * SUB + (SUB - 1)
    )
    attn_ref[...] = dot(last, back_ref[:, :lat]).astype(bf16)


def vmem():
    return pl.BlockSpec(memory_space=pltpu.VMEM)


def smem():
    return pl.BlockSpec(memory_space=pltpu.SMEM)


def hbm():
    return pl.BlockSpec(memory_space=pltpu.HBM)


def in_hbm(*arrays):
    return [pltpu.with_memory_space_constraint(a, pltpu.HBM) for a in arrays]


def in_vmem(*arrays):
    return [pltpu.with_memory_space_constraint(a, pltpu.VMEM) for a in arrays]


def call(kernel, out_shape, in_specs, scratch=(), vmem_mib=32):
    several = isinstance(out_shape, (tuple, list))
    return pl.pallas_call(
        kernel,
        out_shape=out_shape,
        in_specs=in_specs,
        out_specs=tuple(vmem() for _ in out_shape) if several else vmem(),
        scratch_shapes=list(scratch),
        compiler_params=pltpu.CompilerParams(vmem_limit_bytes=vmem_mib << 20),
    )


def local(
    hidden_in,
    batch_len,
    expert_ids,
    gate_num,
    w_gate,
    w_up,
    w_down,
    q_latent,
    q_rope,
    kv_latent,
    kv_rope,
    ctx_len,
):
    owners = lax.axis_size("expert")
    tok, features = hidden_in.shape
    half = features // 2
    hidden_units = w_gate.shape[2]
    batch, heads, lat = q_latent.shape
    total_rows = owners * SUB
    slots = CAP * owners
    width = CAP * half // (SUB - 1)
    tensor = lax.axis_index("tensor")
    swap = [(0, 1), (1, 0)]

    def exchanged(packed):
        whole = packed.reshape(owners, SUB, width)
        return lax.all_to_all(whole, "expert", 0, 0, tiled=True).reshape(total_rows, width)

    ids_t, gate_t = expert_ids.T, gate_num.T
    arrays = (hidden_in, ids_t, q_latent, q_rope, kv_latent, kv_rope)
    half_down = pltpu.VMEM((hidden_units, half), bf16)
    packed, given = call(
        pack_kernel,
        (pltpu.VMEM((total_rows, width), bf16), half_down),
        [smem()] + [hbm() for _ in range(8)],
        [pltpu.SMEM(ctx_len.shape, ctx_len.dtype)]
        + [pltpu.VMEM(a.shape, a.dtype) for a in arrays]
        + [pltpu.SemaphoreType.DMA((8,))],
    )(batch_len, *in_hbm(ctx_len, *arrays, w_down))
    own = exchanged(packed)
    other = lax.ppermute(own, "tensor", swap)
    down_other = lax.ppermute(given, "tensor", swap)
    partial = jax.ShapeDtypeStruct((slots, hidden_units), f32)
    half_up = pltpu.VMEM((half, hidden_units), bf16)
    gate, upper, attn, next_up = call(
        own_kernel,
        (partial, partial, jax.ShapeDtypeStruct((16, lat), bf16), half_up),
        [vmem(), vmem(), hbm()],
        [half_up, pltpu.VMEM((slots, half), bf16), pltpu.SemaphoreType.DMA((2,))],
    )(own, w_gate, *in_hbm(w_up))
    hidden = call(
        other_kernel,
        jax.ShapeDtypeStruct((slots, hidden_units), bf16),
        [vmem() for _ in range(5)],
        [pltpu.VMEM((slots, half), bf16)],
    )(other, w_gate, *in_vmem(next_up), gate, upper)
    hidden_other = lax.ppermute(hidden, "tensor", swap)
    weights = call(
        weigh_kernel,
        jax.ShapeDtypeStruct((2 * CAP, SUB * tok, total_rows), bf16),
        [vmem(), smem(), vmem(), vmem()],
    )(hidden, batch_len, ids_t, gate_t)
    summed = call(
        down_kernel,
        jax.ShapeDtypeStruct((slots, half), f32),
        [vmem(), vmem(), vmem()],
    )(hidden, w_down, weights)
    returned = call(
        back_kernel,
        jax.ShapeDtypeStruct((total_rows, width), bf16),
        [vmem() for _ in range(4)],
        [pltpu.VMEM((total_rows // BLOCKS, width), bf16)],
    )(summed, hidden_other, *in_vmem(down_other), attn)
    back = exchanged(returned)
    moe_half, attn_out = call(
        sum_kernel,
        (
            jax.ShapeDtypeStruct((tok, half), bf16),
            pltpu.VMEM((batch * heads, lat), bf16),
        ),
        [vmem(), vmem()],
    )(weights, back)
    moe_other = lax.ppermute(moe_half, "tensor", swap)
    moe_out = jnp.where(
        tensor == 0,
        jnp.concatenate([moe_half, moe_other], axis=1),
        jnp.concatenate([moe_other, moe_half], axis=1),
    )
    return moe_out, attn_out.reshape(batch, heads, lat)


def solution(mesh):
    both = ("groups", "expert")
    in_specs = (
        P(both, None),
        P("groups"),
        P(both, None),
        P(both, None),
        P("expert", None, "tensor"),
        P("expert", None, "tensor"),
        P("expert", "tensor", None),
        P("groups", "tensor", None),
        P("groups", "tensor", None),
        P("groups", "expert", None),
        P("groups", None, "expert"),
        P("groups"),
    )
    out_specs = (P(both, None), P("groups", "tensor", None))
    return jax.shard_map(local, mesh=mesh, in_specs=in_specs, out_specs=out_specs, check_vma=False)
```

```python
import jax
import jax.numpy as jnp
from jax import lax
from jax.experimental import pallas as pl
from jax.experimental.pallas import tpu as pltpu
from jax.sharding import PartitionSpec as P

SUB = 8
CAP = 3
bf16 = jnp.bfloat16
f32 = jnp.float32
softmax_scale = 192.0 ** (-0.5)
gate_denominator = 1024.0
BLOCKS = 2
PACK_COST = pl.CostEstimate(flops=20_000_000_000, bytes_accessed=16_000_000, transcendentals=0)


def iota(shape, dim):
    return lax.broadcasted_iota(jnp.int32, shape, dim)


def dot(a, b):
    return jnp.dot(a, b, preferred_element_type=f32)


def dot_nt(a, b):
    return lax.dot_general(a, b, (((1,), (1,)), ((), ())), preferred_element_type=f32)


def ones_where(condition, dtype=bf16):
    return jnp.where(condition, 1.0, 0.0).astype(dtype)


def in_three(value):
    high = value.astype(bf16).astype(f32)
    middle = (value - high).astype(bf16).astype(f32)
    return high, middle, (value - high - middle).astype(bf16).astype(f32)


def routing(ids_t, owners, tok, live_count):
    topk = ids_t.shape[0]
    lanes = SUB * tok
    repeat = ones_where(iota((tok, lanes), 1) % tok == iota((tok, lanes), 0))
    ids = dot(ids_t.astype(f32).astype(bf16), repeat)
    row = iota((owners, lanes), 0).astype(f32)
    picks = [ids[k : k + 1, :] == row for k in range(topk)]
    live = lax.axis_index("expert") * tok + iota((owners, lanes), 1) % tok < live_count
    match = sum(ones_where(p, f32) for p in picks)
    match = jnp.where(live, match, 0.0)
    first, second = iota((lanes, lanes), 0), iota((lanes, lanes), 1)
    before = ones_where((first // tok == second // tok) & (first < second))
    return repeat, picks, match, dot(match.astype(bf16), before)


def pack_kernel(
    len_ref, ctx_hbm, hid_hbm, ids_hbm, ql_hbm, qr_hbm, kl_hbm, kr_hbm, wd_hbm,
    out_ref, give_ref,
    ctx_ref, hid_ref, ids_ref, ql_ref, qr_ref, kl_ref, kr_ref, sems,
):
    expert, tensor = lax.axis_index("expert"), lax.axis_index("tensor")
    half = hid_ref.shape[1] // 2
    mine = pl.ds(pl.multiple_of(tensor * half, half), half)
    theirs = pl.ds(pl.multiple_of((1 - tensor) * half, half), half)
    copies = copied(
        (
            (ql_hbm, ql_ref), (kl_hbm, kl_ref), (qr_hbm, qr_ref), (kr_hbm, kr_ref),
            (ctx_hbm, ctx_ref), (ids_hbm, ids_ref), (hid_hbm, hid_ref),
            (wd_hbm.at[0, :, theirs], give_ref),
        ),
        sems,
    )
    total_rows, width = out_ref.shape
    owners = total_rows // SUB
    piece = width // CAP
    tok = hid_ref.shape[0]
    batch, heads, lat = ql_ref.shape
    ctx_dev = kl_ref.shape[1]

    block = SUB * tok
    sub, lane = iota((SUB, block), 0), iota((SUB, block), 1)
    kept = (sub == lane // tok) & (lane < block - tok)
    last = ones_where(
        iota((total_rows, owners), 0) == iota((total_rows, owners), 1) * SUB + (SUB - 1)
    )
    for copy in copies[:7]:
        copy.wait()
    parts = []
    for b in range(batch):
        latent = kl_ref[b]
        s = dot_nt(ql_ref[b], latent) + dot(qr_ref[b], kr_ref[b])
        valid = expert * ctx_dev + iota((heads, ctx_dev), 1) < ctx_ref[b]
        s = jnp.where(valid, s * softmax_scale, -1e30)
        top = jnp.max(s, axis=1, keepdims=True)
        p = jnp.where(valid, jnp.exp(s - top), 0.0)
        total = jnp.sum(p, axis=1, keepdims=True)
        mean = dot(p.astype(bf16), latent) / jnp.where(total > 0.0, total, 1.0)
        at = iota((heads, width - lat), 1)
        stats = jnp.zeros((heads, width - lat), f32)
        for k, number in enumerate(in_three(top) + in_three(total)):
            stats = jnp.where(at == k, number, stats)
        parts.append(jnp.concatenate([mean, stats], axis=1).astype(bf16))
    attn = jnp.concatenate(parts, axis=0)

    _, _, match, rank = routing(ids_ref[...], owners, tok, len_ref[0])
    hidden = hid_ref[...]
    source = jnp.where(tensor == 0, hidden[:, :half], hidden[:, half:])
    stacked = [source[:, k * piece : (k + 1) * piece] for k in range(half // piece)]
    stacked.append(jnp.zeros((tok, piece), bf16))
    stacked = jnp.concatenate(stacked, axis=0)
    for c in range(CAP):
        mine = jnp.where(rank == c, match, 0.0)
        lhs = jnp.where(kept, mine[:, None, :], 0.0).reshape(total_rows, block).astype(bf16)
        at = slice(c * piece, (c + 1) * piece)
        lhs = jnp.concatenate([lhs, last], axis=1)
        rhs = jnp.concatenate([stacked, attn[:, at]], axis=0)
        out_ref[:, at] = dot(lhs, rhs).astype(bf16)
    for copy in copies[7:]:
        copy.wait()


def sort_rows(arrived, rows):
    total_rows, width = arrived.shape
    owners = total_rows // SUB
    piece = width // CAP
    part = owners // BLOCKS
    size = SUB * part
    row, col = iota((size, size), 0), iota((size, size), 1)
    order = ones_where(col == (row % part) * SUB + row // part)
    attention = []
    for b in range(BLOCKS):
        ordered = dot(order, arrived[b * size : (b + 1) * size])
        for k in range(SUB - 1):
            for c in range(CAP):
                first = c * owners + b * part
                rows[first : first + part, k * piece : (k + 1) * piece] = ordered[
                    k * part : (k + 1) * part, c * piece : (c + 1) * piece
                ].astype(bf16)
        attention.append(ordered[size - part :])
    return jnp.concatenate(attention, axis=0)


def copied(pairs, sems):
    copies = [pltpu.make_async_copy(a, b, sems.at[k]) for k, (a, b) in enumerate(pairs)]
    for copy in copies:
        copy.start()
    return copies


def own_kernel(own_ref, wg_ref, wu_ref, gate_ref, upper_ref, attn_ref, rows):
    half = rows.shape[1]
    lat = attn_ref.shape[1]
    mine = pl.ds(pl.multiple_of(lax.axis_index("tensor") * half, half), half)
    arrived = sort_rows(own_ref[...], rows)
    stats = [arrived[:, lat + k : lat + k + 1] for k in range(6)]
    top = stats[0] + stats[1] + stats[2]
    total = stats[3] + stats[4] + stats[5]
    share = jnp.exp(top - jnp.max(top, axis=0, keepdims=True)) * total
    weighted = jnp.sum(share * arrived[:, :lat], axis=0, keepdims=True)
    done = weighted / jnp.sum(share, axis=0, keepdims=True)
    attn_ref[...] = jnp.broadcast_to(done, attn_ref.shape).astype(bf16)
    gate_ref[...] = dot(rows[...], wg_ref[0, mine, :])
    upper_ref[...] = dot(rows[...], wu_ref[0, mine, :])


def other_kernel(other_ref, wg_ref, wu_ref, gate_ref, upper_ref, hidden_ref, rows):
    half = rows.shape[1]
    theirs = pl.ds(pl.multiple_of((1 - lax.axis_index("tensor")) * half, half), half)
    sort_rows(other_ref[...], rows)
    gate = gate_ref[...] + dot(rows[...], wg_ref[0, theirs, :])
    upper = upper_ref[...] + dot(rows[...], wu_ref[0, theirs, :])
    hidden_ref[...] = (gate / (1.0 + jnp.exp(-gate)) * upper).astype(bf16)


def weigh_kernel(hidden_ref, len_ref, ids_ref, gate_ref, weigh_ref):
    weigh(len_ref, ids_ref, gate_ref, weigh_ref)


def down_kernel(hidden_ref, wd_ref, weigh_ref, sum_ref):
    half = sum_ref.shape[1]
    mine = pl.ds(pl.multiple_of(lax.axis_index("tensor") * half, half), half)
    sum_ref[...] = dot(hidden_ref[...], wd_ref[0, :, mine])


def back_kernel(sum_ref, hidden_ref, wd_ref, attn_ref, out_ref, rows):
    total_rows, width = out_ref.shape
    owners = total_rows // SUB
    piece = width // CAP
    lat = attn_ref.shape[1]
    whole = (sum_ref[...] + dot(hidden_ref[...], wd_ref[...])).astype(bf16)
    part = owners // BLOCKS
    size = SUB * part
    row, col = iota((size, size), 0), iota((size, size), 1)
    order = ones_where(col == (row % SUB) * part + row // SUB)
    rows[size - part :, :lat] = jnp.broadcast_to(attn_ref[0:1, :], (part, lat))
    rows[size - part :, lat:] = jnp.zeros((part, width - lat), bf16)
    for b in range(BLOCKS):
        for k in range(SUB - 1):
            for c in range(CAP):
                first = c * owners + b * part
                rows[k * part : (k + 1) * part, c * piece : (c + 1) * piece] = whole[
                    first : first + part, k * piece : (k + 1) * piece
                ]
        out_ref[b * size : (b + 1) * size, :] = dot(order, rows[...]).astype(bf16)


def weigh(len_ref, ids_ref, gate_ref, weigh_ref):
    tok = ids_ref.shape[1]
    block, total_rows = SUB * tok, weigh_ref.shape[2]
    owners = total_rows // SUB
    repeat, picks, match, rank = routing(ids_ref[...], owners, tok, len_ref[0])
    gates = gate_ref[...]
    lower = gates % 8
    split = []
    for number in (gates - lower, lower):
        number = dot(number.astype(f32).astype(bf16), repeat)
        split.append(sum(jnp.where(p, number[k : k + 1, :], 0.0) for k, p in enumerate(picks)))
    spread = ones_where(iota((owners, total_rows), 1) // SUB == iota((owners, total_rows), 0))
    row, col = iota((block, total_rows), 0), iota((block, total_rows), 1)
    kept = row // tok == col % SUB
    for c in range(CAP):
        for n, number in enumerate(split):
            mine = jnp.where((rank == c) & (match > 0.0), number, 0.0)
            weigh_ref[2 * c + n] = jnp.where(kept, dot(mine.T.astype(bf16), spread), 0.0).astype(bf16)


def sum_kernel(weigh_ref, back_ref, moe_ref, attn_ref):
    total_rows, width = back_ref.shape
    owners = total_rows // SUB
    piece = width // CAP
    tok, _ = moe_ref.shape
    summed = sum(
        dot(weigh_ref[2 * c + n], back_ref[:, c * piece : (c + 1) * piece])
        for c in range(CAP)
        for n in range(2)
    ) * (1.0 / gate_denominator)
    for k in range(SUB - 1):
        moe_ref[:, k * piece : (k + 1) * piece] = summed[k * tok : (k + 1) * tok].astype(bf16)
    lat = attn_ref.shape[1]
    last = ones_where(
        iota((owners, total_rows), 1) == iota((owners, total_rows), 0) * SUB + (SUB - 1)
    )
    attn_ref[...] = dot(last, back_ref[:, :lat]).astype(bf16)


def vmem():
    return pl.BlockSpec(memory_space=pltpu.VMEM)


def smem():
    return pl.BlockSpec(memory_space=pltpu.SMEM)


def hbm():
    return pl.BlockSpec(memory_space=pltpu.HBM)


def in_hbm(*arrays):
    return [pltpu.with_memory_space_constraint(a, pltpu.HBM) for a in arrays]


def in_vmem(*arrays):
    return [pltpu.with_memory_space_constraint(a, pltpu.VMEM) for a in arrays]


def call(kernel, out_shape, in_specs, scratch=(), vmem_mib=32, cost=None):
    several = isinstance(out_shape, (tuple, list))
    return pl.pallas_call(
        kernel,
        out_shape=out_shape,
        in_specs=in_specs,
        out_specs=tuple(vmem() for _ in out_shape) if several else vmem(),
        scratch_shapes=list(scratch),
        compiler_params=pltpu.CompilerParams(vmem_limit_bytes=vmem_mib << 20),
        cost_estimate=cost,
    )


def local(
    hidden_in,
    batch_len,
    expert_ids,
    gate_num,
    w_gate,
    w_up,
    w_down,
    q_latent,
    q_rope,
    kv_latent,
    kv_rope,
    ctx_len,
):
    owners = lax.axis_size("expert")
    tok, features = hidden_in.shape
    half = features // 2
    hidden_units = w_gate.shape[2]
    batch, heads, lat = q_latent.shape
    total_rows = owners * SUB
    slots = CAP * owners
    width = CAP * half // (SUB - 1)
    tensor = lax.axis_index("tensor")
    swap = [(0, 1), (1, 0)]

    def exchanged(packed):
        whole = packed.reshape(owners, SUB, width)
        return lax.all_to_all(whole, "expert", 0, 0, tiled=True).reshape(total_rows, width)

    ids_t, gate_t = expert_ids.T, gate_num.T
    arrays = (hidden_in, ids_t, q_latent, q_rope, kv_latent, kv_rope)
    half_down = pltpu.VMEM((hidden_units, half), bf16)
    packed, given = call(
        pack_kernel,
        (pltpu.VMEM((total_rows, width), bf16), half_down),
        [smem()] + [hbm() for _ in range(8)],
        [pltpu.SMEM(ctx_len.shape, ctx_len.dtype)]
        + [pltpu.VMEM(a.shape, a.dtype) for a in arrays]
        + [pltpu.SemaphoreType.DMA((8,))],
        cost=PACK_COST,
    )(batch_len, *in_hbm(ctx_len, *arrays, w_down))
    own = exchanged(packed)
    other = lax.ppermute(own, "tensor", swap)
    down_other = lax.ppermute(given, "tensor", swap)
    partial = jax.ShapeDtypeStruct((slots, hidden_units), f32)
    gate, upper, attn = call(
        own_kernel,
        (partial, partial, jax.ShapeDtypeStruct((16, lat), bf16)),
        [vmem(), vmem(), vmem()],
        [pltpu.VMEM((slots, half), bf16)],
    )(own, w_gate, w_up)
    hidden = call(
        other_kernel,
        jax.ShapeDtypeStruct((slots, hidden_units), bf16),
        [vmem() for _ in range(5)],
        [pltpu.VMEM((slots, half), bf16)],
    )(other, w_gate, w_up, gate, upper)
    hidden_other = lax.ppermute(hidden, "tensor", swap)
    weights = call(
        weigh_kernel,
        jax.ShapeDtypeStruct((2 * CAP, SUB * tok, total_rows), bf16),
        [vmem(), smem(), vmem(), vmem()],
    )(hidden, batch_len, ids_t, gate_t)
    summed = call(
        down_kernel,
        jax.ShapeDtypeStruct((slots, half), f32),
        [vmem(), vmem(), vmem()],
    )(hidden, w_down, weights)
    returned = call(
        back_kernel,
        jax.ShapeDtypeStruct((total_rows, width), bf16),
        [vmem() for _ in range(4)],
        [pltpu.VMEM((total_rows // BLOCKS, width), bf16)],
    )(summed, hidden_other, *in_vmem(down_other), attn)
    back = exchanged(returned)
    moe_half, attn_out = call(
        sum_kernel,
        (
            jax.ShapeDtypeStruct((tok, half), bf16),
            pltpu.VMEM((batch * heads, lat), bf16),
        ),
        [vmem(), vmem()],
    )(weights, back)
    moe_other = lax.ppermute(moe_half, "tensor", swap)
    moe_out = jnp.where(
        tensor == 0,
        jnp.concatenate([moe_half, moe_other], axis=1),
        jnp.concatenate([moe_other, moe_half], axis=1),
    )
    return moe_out, attn_out.reshape(batch, heads, lat)


def solution(mesh):
    both = ("groups", "expert")
    in_specs = (
        P(both, None),
        P("groups"),
        P(both, None),
        P(both, None),
        P("expert", None, "tensor"),
        P("expert", None, "tensor"),
        P("expert", "tensor", None),
        P("groups", "tensor", None),
        P("groups", "tensor", None),
        P("groups", "expert", None),
        P("groups", None, "expert"),
        P("groups"),
    )
    out_specs = (P(both, None), P("groups", "tensor", None))
    return jax.shard_map(local, mesh=mesh, in_specs=in_specs, out_specs=out_specs, check_vma=False)
```

```python
import jax
import jax.numpy as jnp
from jax import lax
from jax.experimental import pallas as pl
from jax.experimental.pallas import tpu as pltpu
from jax.sharding import PartitionSpec as P

SUB = 8
CAP = 3
bf16 = jnp.bfloat16
f32 = jnp.float32
softmax_scale = 192.0 ** (-0.5)
gate_denominator = 1024.0
BLOCKS = 2
PACK_COST = pl.CostEstimate(flops=20_000_000_000, bytes_accessed=16_000_000, transcendentals=0)


def iota(shape, dim):
    return lax.broadcasted_iota(jnp.int32, shape, dim)


def dot(a, b):
    return jnp.dot(a, b, preferred_element_type=f32)


def dot_nt(a, b):
    return lax.dot_general(a, b, (((1,), (1,)), ((), ())), preferred_element_type=f32)


def ones_where(condition, dtype=bf16):
    return jnp.where(condition, 1.0, 0.0).astype(dtype)


def in_three(value):
    high = value.astype(bf16).astype(f32)
    middle = (value - high).astype(bf16).astype(f32)
    return high, middle, (value - high - middle).astype(bf16).astype(f32)


def routing(ids_t, owners, tok, live_count):
    topk = ids_t.shape[0]
    lanes = SUB * tok
    repeat = ones_where(iota((tok, lanes), 1) % tok == iota((tok, lanes), 0))
    ids = dot(ids_t.astype(f32).astype(bf16), repeat)
    row = iota((owners, lanes), 0).astype(f32)
    picks = [ids[k : k + 1, :] == row for k in range(topk)]
    live = lax.axis_index("expert") * tok + iota((owners, lanes), 1) % tok < live_count
    match = sum(ones_where(p, f32) for p in picks)
    match = jnp.where(live, match, 0.0)
    first, second = iota((lanes, lanes), 0), iota((lanes, lanes), 1)
    before = ones_where((first // tok == second // tok) & (first < second))
    return repeat, picks, match, dot(match.astype(bf16), before)


def pack_kernel(
    len_ref, ctx_hbm, hid_hbm, ids_hbm, ql_hbm, qr_hbm, kl_hbm, kr_hbm, wd_hbm,
    out_ref, give_ref,
    ctx_ref, hid_ref, ids_ref, ql_ref, qr_ref, kl_ref, kr_ref, sems,
):
    expert, tensor = lax.axis_index("expert"), lax.axis_index("tensor")
    half = hid_ref.shape[1] // 2
    mine = pl.ds(pl.multiple_of(tensor * half, half), half)
    theirs = pl.ds(pl.multiple_of((1 - tensor) * half, half), half)
    copies = copied(
        (
            (ql_hbm, ql_ref), (kl_hbm, kl_ref), (qr_hbm, qr_ref), (kr_hbm, kr_ref),
            (ctx_hbm, ctx_ref), (ids_hbm, ids_ref), (hid_hbm, hid_ref),
            (wd_hbm.at[0, :, theirs], give_ref),
        ),
        sems,
    )
    total_rows, width = out_ref.shape
    owners = total_rows // SUB
    piece = width // CAP
    tok = hid_ref.shape[0]
    batch, heads, lat = ql_ref.shape
    ctx_dev = kl_ref.shape[1]

    block = SUB * tok
    sub, lane = iota((SUB, block), 0), iota((SUB, block), 1)
    kept = (sub == lane // tok) & (lane < block - tok)
    last = ones_where(
        iota((total_rows, owners), 0) == iota((total_rows, owners), 1) * SUB + (SUB - 1)
    )
    for copy in copies[:7]:
        copy.wait()
    parts = []
    for b in range(batch):
        latent = kl_ref[b]
        s = dot_nt(ql_ref[b], latent) + dot(qr_ref[b], kr_ref[b])
        valid = expert * ctx_dev + iota((heads, ctx_dev), 1) < ctx_ref[b]
        s = jnp.where(valid, s * softmax_scale, -1e30)
        top = jnp.max(s, axis=1, keepdims=True)
        p = jnp.where(valid, jnp.exp(s - top), 0.0)
        total = jnp.sum(p, axis=1, keepdims=True)
        mean = dot(p.astype(bf16), latent) / jnp.where(total > 0.0, total, 1.0)
        at = iota((heads, width - lat), 1)
        stats = jnp.zeros((heads, width - lat), f32)
        for k, number in enumerate(in_three(top) + in_three(total)):
            stats = jnp.where(at == k, number, stats)
        parts.append(jnp.concatenate([mean, stats], axis=1).astype(bf16))
    attn = jnp.concatenate(parts, axis=0)

    _, _, match, rank = routing(ids_ref[...], owners, tok, len_ref[0])
    hidden = hid_ref[...]
    source = jnp.where(tensor == 0, hidden[:, :half], hidden[:, half:])
    stacked = [source[:, k * piece : (k + 1) * piece] for k in range(half // piece)]
    stacked.append(jnp.zeros((tok, piece), bf16))
    stacked = jnp.concatenate(stacked, axis=0)
    for c in range(CAP):
        mine = jnp.where(rank == c, match, 0.0)
        lhs = jnp.where(kept, mine[:, None, :], 0.0).reshape(total_rows, block).astype(bf16)
        at = slice(c * piece, (c + 1) * piece)
        lhs = jnp.concatenate([lhs, last], axis=1)
        rhs = jnp.concatenate([stacked, attn[:, at]], axis=0)
        out_ref[:, at] = dot(lhs, rhs).astype(bf16)
    for copy in copies[7:]:
        copy.wait()


def sort_rows(arrived, rows):
    total_rows, width = arrived.shape
    owners = total_rows // SUB
    piece = width // CAP
    part = owners // BLOCKS
    size = SUB * part
    row, col = iota((size, size), 0), iota((size, size), 1)
    order = ones_where(col == (row % part) * SUB + row // part)
    attention = []
    for b in range(BLOCKS):
        ordered = dot(order, arrived[b * size : (b + 1) * size])
        for k in range(SUB - 1):
            for c in range(CAP):
                first = c * owners + b * part
                rows[first : first + part, k * piece : (k + 1) * piece] = ordered[
                    k * part : (k + 1) * part, c * piece : (c + 1) * piece
                ].astype(bf16)
        attention.append(ordered[size - part :])
    return jnp.concatenate(attention, axis=0)


def copied(pairs, sems):
    copies = [pltpu.make_async_copy(a, b, sems.at[k]) for k, (a, b) in enumerate(pairs)]
    for copy in copies:
        copy.start()
    return copies


def own_kernel(own_ref, wg_ref, wu_ref, gate_ref, upper_ref, attn_ref, rows):
    half = rows.shape[1]
    lat = attn_ref.shape[1]
    mine = pl.ds(pl.multiple_of(lax.axis_index("tensor") * half, half), half)
    arrived = sort_rows(own_ref[...], rows)
    stats = [arrived[:, lat + k : lat + k + 1] for k in range(6)]
    top = stats[0] + stats[1] + stats[2]
    total = stats[3] + stats[4] + stats[5]
    share = jnp.exp(top - jnp.max(top, axis=0, keepdims=True)) * total
    weighted = jnp.sum(share * arrived[:, :lat], axis=0, keepdims=True)
    done = weighted / jnp.sum(share, axis=0, keepdims=True)
    attn_ref[...] = jnp.broadcast_to(done, attn_ref.shape).astype(bf16)
    gate_ref[...] = dot(rows[...], wg_ref[0, mine, :])
    upper_ref[...] = dot(rows[...], wu_ref[0, mine, :])


def other_kernel(other_ref, wg_ref, wu_ref, gate_ref, upper_ref, weigh_ref, hidden_ref, rows):
    half = rows.shape[1]
    theirs = pl.ds(pl.multiple_of((1 - lax.axis_index("tensor")) * half, half), half)
    sort_rows(other_ref[...], rows)
    gate = gate_ref[...] + dot(rows[...], wg_ref[0, theirs, :])
    upper = upper_ref[...] + dot(rows[...], wu_ref[0, theirs, :])
    hidden_ref[...] = (gate / (1.0 + jnp.exp(-gate)) * upper).astype(bf16)


def weigh_kernel(after_ref, len_ref, ids_ref, gate_ref, weigh_ref):
    weigh(len_ref, ids_ref, gate_ref, weigh_ref)


def down_kernel(hidden_ref, wd_ref, sum_ref):
    half = sum_ref.shape[1]
    mine = pl.ds(pl.multiple_of(lax.axis_index("tensor") * half, half), half)
    sum_ref[...] = dot(hidden_ref[...], wd_ref[0, :, mine])


def back_kernel(sum_ref, hidden_ref, wd_ref, attn_ref, out_ref, rows):
    total_rows, width = out_ref.shape
    owners = total_rows // SUB
    piece = width // CAP
    lat = attn_ref.shape[1]
    whole = (sum_ref[...] + dot(hidden_ref[...], wd_ref[...])).astype(bf16)
    part = owners // BLOCKS
    size = SUB * part
    row, col = iota((size, size), 0), iota((size, size), 1)
    order = ones_where(col == (row % SUB) * part + row // SUB)
    rows[size - part :, :lat] = jnp.broadcast_to(attn_ref[0:1, :], (part, lat))
    rows[size - part :, lat:] = jnp.zeros((part, width - lat), bf16)
    for b in range(BLOCKS):
        for k in range(SUB - 1):
            for c in range(CAP):
                first = c * owners + b * part
                rows[k * part : (k + 1) * part, c * piece : (c + 1) * piece] = whole[
                    first : first + part, k * piece : (k + 1) * piece
                ]
        out_ref[b * size : (b + 1) * size, :] = dot(order, rows[...]).astype(bf16)


def weigh(len_ref, ids_ref, gate_ref, weigh_ref):
    tok = ids_ref.shape[1]
    block, total_rows = SUB * tok, weigh_ref.shape[2]
    owners = total_rows // SUB
    repeat, picks, match, rank = routing(ids_ref[...], owners, tok, len_ref[0])
    gates = gate_ref[...]
    lower = gates % 8
    split = []
    for number in (gates - lower, lower):
        number = dot(number.astype(f32).astype(bf16), repeat)
        split.append(sum(jnp.where(p, number[k : k + 1, :], 0.0) for k, p in enumerate(picks)))
    spread = ones_where(iota((owners, total_rows), 1) // SUB == iota((owners, total_rows), 0))
    row, col = iota((block, total_rows), 0), iota((block, total_rows), 1)
    kept = row // tok == col % SUB
    for c in range(CAP):
        for n, number in enumerate(split):
            mine = jnp.where((rank == c) & (match > 0.0), number, 0.0)
            weigh_ref[2 * c + n] = jnp.where(kept, dot(mine.T.astype(bf16), spread), 0.0).astype(bf16)


def sum_kernel(weigh_ref, back_ref, moe_ref, attn_ref):
    total_rows, width = back_ref.shape
    owners = total_rows // SUB
    piece = width // CAP
    tok, _ = moe_ref.shape
    summed = sum(
        dot(weigh_ref[2 * c + n], back_ref[:, c * piece : (c + 1) * piece])
        for c in range(CAP)
        for n in range(2)
    ) * (1.0 / gate_denominator)
    for k in range(SUB - 1):
        moe_ref[:, k * piece : (k + 1) * piece] = summed[k * tok : (k + 1) * tok].astype(bf16)
    lat = attn_ref.shape[1]
    last = ones_where(
        iota((owners, total_rows), 1) == iota((owners, total_rows), 0) * SUB + (SUB - 1)
    )
    attn_ref[...] = dot(last, back_ref[:, :lat]).astype(bf16)


def vmem():
    return pl.BlockSpec(memory_space=pltpu.VMEM)


def smem():
    return pl.BlockSpec(memory_space=pltpu.SMEM)


def hbm():
    return pl.BlockSpec(memory_space=pltpu.HBM)


def in_hbm(*arrays):
    return [pltpu.with_memory_space_constraint(a, pltpu.HBM) for a in arrays]


def in_vmem(*arrays):
    return [pltpu.with_memory_space_constraint(a, pltpu.VMEM) for a in arrays]


def call(kernel, out_shape, in_specs, scratch=(), vmem_mib=32, cost=None):
    several = isinstance(out_shape, (tuple, list))
    return pl.pallas_call(
        kernel,
        out_shape=out_shape,
        in_specs=in_specs,
        out_specs=tuple(vmem() for _ in out_shape) if several else vmem(),
        scratch_shapes=list(scratch),
        compiler_params=pltpu.CompilerParams(vmem_limit_bytes=vmem_mib << 20),
        cost_estimate=cost,
    )


def local(
    hidden_in,
    batch_len,
    expert_ids,
    gate_num,
    w_gate,
    w_up,
    w_down,
    q_latent,
    q_rope,
    kv_latent,
    kv_rope,
    ctx_len,
):
    owners = lax.axis_size("expert")
    tok, features = hidden_in.shape
    half = features // 2
    hidden_units = w_gate.shape[2]
    batch, heads, lat = q_latent.shape
    total_rows = owners * SUB
    slots = CAP * owners
    width = CAP * half // (SUB - 1)
    tensor = lax.axis_index("tensor")
    swap = [(0, 1), (1, 0)]

    def exchanged(packed):
        whole = packed.reshape(owners, SUB, width)
        return lax.all_to_all(whole, "expert", 0, 0, tiled=True).reshape(total_rows, width)

    ids_t, gate_t = expert_ids.T, gate_num.T
    arrays = (hidden_in, ids_t, q_latent, q_rope, kv_latent, kv_rope)
    half_down = pltpu.VMEM((hidden_units, half), bf16)
    packed, given = call(
        pack_kernel,
        (pltpu.VMEM((total_rows, width), bf16), half_down),
        [smem()] + [hbm() for _ in range(8)],
        [pltpu.SMEM(ctx_len.shape, ctx_len.dtype)]
        + [pltpu.VMEM(a.shape, a.dtype) for a in arrays]
        + [pltpu.SemaphoreType.DMA((8,))],
        cost=PACK_COST,
    )(batch_len, *in_hbm(ctx_len, *arrays, w_down))
    own = exchanged(packed)
    other = lax.ppermute(own, "tensor", swap)
    down_other = lax.ppermute(given, "tensor", swap)
    partial = jax.ShapeDtypeStruct((slots, hidden_units), f32)
    gate, upper, attn = call(
        own_kernel,
        (partial, partial, jax.ShapeDtypeStruct((16, lat), bf16)),
        [vmem(), vmem(), vmem()],
        [pltpu.VMEM((slots, half), bf16)],
    )(own, w_gate, w_up)
    weights = call(
        weigh_kernel,
        jax.ShapeDtypeStruct((2 * CAP, SUB * tok, total_rows), bf16),
        [vmem(), smem(), vmem(), vmem()],
    )(gate, batch_len, ids_t, gate_t)
    hidden = call(
        other_kernel,
        jax.ShapeDtypeStruct((slots, hidden_units), bf16),
        [vmem() for _ in range(6)],
        [pltpu.VMEM((slots, half), bf16)],
    )(other, w_gate, w_up, gate, upper, weights)
    hidden_other = lax.ppermute(hidden, "tensor", swap)
    summed = call(
        down_kernel,
        jax.ShapeDtypeStruct((slots, half), f32),
        [vmem(), vmem()],
    )(hidden, w_down)
    returned = call(
        back_kernel,
        jax.ShapeDtypeStruct((total_rows, width), bf16),
        [vmem() for _ in range(4)],
        [pltpu.VMEM((total_rows // BLOCKS, width), bf16)],
    )(summed, hidden_other, *in_vmem(down_other), attn)
    back = exchanged(returned)
    moe_half, attn_out = call(
        sum_kernel,
        (
            jax.ShapeDtypeStruct((tok, half), bf16),
            pltpu.VMEM((batch * heads, lat), bf16),
        ),
        [vmem(), vmem()],
    )(weights, back)
    moe_other = lax.ppermute(moe_half, "tensor", swap)
    moe_out = jnp.where(
        tensor == 0,
        jnp.concatenate([moe_half, moe_other], axis=1),
        jnp.concatenate([moe_other, moe_half], axis=1),
    )
    return moe_out, attn_out.reshape(batch, heads, lat)


def solution(mesh):
    both = ("groups", "expert")
    in_specs = (
        P(both, None),
        P("groups"),
        P(both, None),
        P(both, None),
        P("expert", None, "tensor"),
        P("expert", None, "tensor"),
        P("expert", "tensor", None),
        P("groups", "tensor", None),
        P("groups", "tensor", None),
        P("groups", "expert", None),
        P("groups", None, "expert"),
        P("groups"),
    )
    out_specs = (P(both, None), P("groups", "tensor", None))
    return jax.shard_map(local, mesh=mesh, in_specs=in_specs, out_specs=out_specs, check_vma=False)
```
